64 devices in a mesh: dp: 4 (over x, y), fsdp: 16 (over z, core).
Axes of the slice: x: 2, y: 2, z: 8, core: 2. Of those that a mesh axis runs over, the one named last changes fastest.
The devices are a block of a 4x4x8 slice.
Arguments:
- hidden: bfloat16 [512, 128, 1024], P(('dp', 'fsdp')), parts along dimension 0
- doc_lens: int32 [512], P(('dp', 'fsdp')), parts along dimension 0
- ln_par: float32 [2, 4, 1024], P(None, None, 'fsdp')
- w_qkv: bfloat16 [2, 1024, 16, 192], P(None, 'fsdp')
- b_qkv: bfloat16 [2, 3072], P(None, 'fsdp')
- w_out: bfloat16 [2, 1024, 1024], P(None, 'fsdp')
- b_out: bfloat16 [2, 1024], P(None, 'fsdp')
- w_up: bfloat16 [2, 1024, 4096], P(None, 'fsdp')
- b_up: bfloat16 [2, 4096], P(None, 'fsdp')
- w_down: bfloat16 [2, 4096, 1024], P(None, 'fsdp')
- b_down: bfloat16 [2, 1024], P(None, 'fsdp')
Outputs:
- output: bfloat16 [512, 128, 1024], P(('dp', 'fsdp')), parts along dimension 0
There are 4 independent parts. The reference program is written for one: setup_inputs(seed, part) draws one part's arguments, and reference() takes and returns one part's arrays. A program takes and returns all parts, laid end to end along the dimension named above; an argument that names none is the same for every part.
All inputs are finite; a program needn't handle non-finite values.
Results may differ from the reference program's by a relative error of at most 0.00929409.
Values are sent between devices in bfloat16 or wider.
A program may use at most 768 MiB of HBM per device.

```python
import jax
import jax.numpy as jnp
from jax import lax

D_MODEL = 1024
NUM_HEADS = 16
HEAD_DIM = 64
FF_DIM = 4096
SEQ_LEN = 128
NUM_DOCS = 128
NUM_LAYERS = 2
ROT_DIM = HEAD_DIM // 4
ROPE_BASE = 10000.0
LN_EPS = 1e-5


def setup_inputs(seed: int = 0, part: int = 0) -> dict:
    shared_key, doc_root = jax.random.split(jax.random.key(seed))
    part_key = jax.random.fold_in(doc_root, part)
    hidden_key, lens_key = jax.random.split(part_key)
    w_keys = jax.random.split(shared_key, 9)
    hidden = jax.random.normal(hidden_key, (NUM_DOCS, SEQ_LEN, D_MODEL), jnp.float32).astype(jnp.bfloat16)
    drawn_lens = jax.random.randint(lens_key, (NUM_DOCS,), 1, SEQ_LEN + 1, jnp.int32)
    doc_lens = drawn_lens.at[0].set(SEQ_LEN)
    ln_offset = jnp.array([1.0, 0.0, 1.0, 0.0], jnp.float32)[None, :, None]
    ln_par = ln_offset + 0.4 * jax.random.normal(w_keys[0], (NUM_LAYERS, 4, D_MODEL), jnp.float32)
    w_qkv = (jax.random.normal(w_keys[1], (NUM_LAYERS, D_MODEL, NUM_HEADS, 3 * HEAD_DIM), jnp.float32) * D_MODEL ** -0.5).astype(jnp.bfloat16)
    b_qkv = (0.5 * jax.random.normal(w_keys[2], (NUM_LAYERS, 3 * D_MODEL), jnp.float32)).astype(jnp.bfloat16)
    w_out = (jax.random.normal(w_keys[3], (NUM_LAYERS, D_MODEL, D_MODEL), jnp.float32) * D_MODEL ** -0.5).astype(jnp.bfloat16)
    b_out = (0.5 * jax.random.normal(w_keys[4], (NUM_LAYERS, D_MODEL), jnp.float32)).astype(jnp.bfloat16)
    w_up = (jax.random.normal(w_keys[5], (NUM_LAYERS, D_MODEL, FF_DIM), jnp.float32) * D_MODEL ** -0.5).astype(jnp.bfloat16)
    b_up = (0.5 * jax.random.normal(w_keys[6], (NUM_LAYERS, FF_DIM), jnp.float32)).astype(jnp.bfloat16)
    w_down = (jax.random.normal(w_keys[7], (NUM_LAYERS, FF_DIM, D_MODEL), jnp.float32) * FF_DIM ** -0.5).astype(jnp.bfloat16)
    b_down = (0.5 * jax.random.normal(w_keys[8], (NUM_LAYERS, D_MODEL), jnp.float32)).astype(jnp.bfloat16)
    return {'hidden': hidden, 'doc_lens': doc_lens, 'ln_par': ln_par, 'w_qkv': w_qkv, 'b_qkv': b_qkv, 'w_out': w_out, 'b_out': b_out, 'w_up': w_up, 'b_up': b_up, 'w_down': w_down, 'b_down': b_down}


def layer_norm(row_vals, gain_vec, shift_vec):
    mean_vals = jnp.mean(row_vals, axis=-1, keepdims=True)
    centered = row_vals - mean_vals
    var_vals = jnp.mean(centered * centered, axis=-1, keepdims=True)
    normed = centered * lax.rsqrt(var_vals + LN_EPS)
    return (normed * gain_vec + shift_vec).astype(jnp.bfloat16)


def rotary_tables(seq_len, rot_dim):
    inv_freq = 1.0 / (ROPE_BASE ** (jnp.arange(0, rot_dim, 2, dtype=jnp.float32) / rot_dim))
    angles = jnp.arange(seq_len, dtype=jnp.float32)[:, None] * inv_freq[None, :]
    angles = jnp.concatenate([angles, angles], axis=-1)
    return jnp.cos(angles), jnp.sin(angles)


def apply_rotary(head_vals, cos_tab, sin_tab):
    half_rot = ROT_DIM // 2
    rot_part = head_vals[..., :ROT_DIM].astype(jnp.float32)
    turned = jnp.concatenate([-rot_part[..., half_rot:], rot_part[..., :half_rot]], axis=-1)
    rotated = rot_part * cos_tab[:, None, :] + turned * sin_tab[:, None, :]
    return jnp.concatenate([rotated.astype(jnp.bfloat16), head_vals[..., ROT_DIM:]], axis=-1)


def doc_forward(doc_hidden, doc_len, layer_params, cos_tab, sin_tab):
    positions = jnp.arange(SEQ_LEN)
    visible = (positions[None, :] <= positions[:, None]) & (positions[None, :] < doc_len)

    def layer_step(x_cur, params):
        ln_rows, w_qkv_l, b_qkv_l, w_out_l, b_out_l, w_up_l, b_up_l, w_down_l, b_down_l = params
        x_rows = x_cur.astype(jnp.float32)
        attn_in = layer_norm(x_rows, ln_rows[0], ln_rows[1])
        mlp_in = layer_norm(x_rows, ln_rows[2], ln_rows[3])
        qkv_rows = jnp.dot(attn_in, w_qkv_l.reshape(D_MODEL, 3 * D_MODEL), preferred_element_type=jnp.float32) + b_qkv_l.astype(jnp.float32)
        qkv_heads = qkv_rows.astype(jnp.bfloat16).reshape(SEQ_LEN, NUM_HEADS, 3 * HEAD_DIM)
        queries = apply_rotary(qkv_heads[:, :, :HEAD_DIM], cos_tab, sin_tab)
        keys_rot = apply_rotary(qkv_heads[:, :, HEAD_DIM:2 * HEAD_DIM], cos_tab, sin_tab)
        values = qkv_heads[:, :, 2 * HEAD_DIM:]
        scores = jnp.einsum('qhe,khe->hqk', queries.astype(jnp.float32), keys_rot.astype(jnp.float32)) * (HEAD_DIM ** -0.5)
        prob_bf = jax.nn.softmax(jnp.where(visible[None], scores, -1e30), axis=-1).astype(jnp.bfloat16)
        context = jnp.einsum('hqk,khe->qhe', prob_bf.astype(jnp.float32), values.astype(jnp.float32))
        context = context.astype(jnp.bfloat16).reshape(SEQ_LEN, D_MODEL)
        attn_out = jnp.dot(context, w_out_l, preferred_element_type=jnp.float32) + b_out_l.astype(jnp.float32)
        up_rows = jnp.dot(mlp_in, w_up_l, preferred_element_type=jnp.float32) + b_up_l.astype(jnp.float32)
        act_rows = jax.nn.gelu(up_rows, approximate=False).astype(jnp.bfloat16)
        mlp_out = jnp.dot(act_rows, w_down_l, preferred_element_type=jnp.float32) + b_down_l.astype(jnp.float32)
        new_x = (x_rows + attn_out + mlp_out).astype(jnp.bfloat16)
        return new_x, None

    return lax.scan(layer_step, doc_hidden, layer_params)[0]


def reference(hidden, doc_lens, ln_par, w_qkv, b_qkv, w_out, b_out, w_up, b_up, w_down, b_down):
    cos_tab, sin_tab = rotary_tables(SEQ_LEN, ROT_DIM)
    layer_params = (ln_par, w_qkv, b_qkv, w_out, b_out, w_up, b_up, w_down, b_down)
    return lax.map(lambda doc_item: doc_forward(doc_item[0], doc_item[1], layer_params, cos_tab, sin_tab), (hidden, doc_lens))
```

```python
import math

import jax
import jax.numpy as jnp
import numpy as np
from jax import lax
from jax.experimental import pallas as pl
from jax.experimental.pallas import tpu as pltpu
from jax.sharding import PartitionSpec as P

MESH = pl.DeviceIdType.MESH
ROPE_BASE = 10000.0
LN_EPS = 1e-5
BF = jnp.bfloat16
F32 = jnp.float32
TILE = 256
STEPS = 4
PAR_ROWS = 16


def rotary_lanes(seq_len, head_dim):
    rot = head_dim // 4
    half = rot // 2
    inv_freq = (1.0 / (ROPE_BASE ** (np.arange(0, rot, 2, dtype=np.float32) / rot))).astype(np.float32)
    angles = np.arange(seq_len, dtype=np.float32)[:, None] * inv_freq[None, :]
    cos_v, sin_v = np.cos(angles), np.sin(angles)
    tab = np.zeros((3, seq_len, 2 * head_dim), np.float32)
    tab[0] = 1.0
    for base in (0, head_dim):
        tab[0, :, base:base + half] = cos_v
        tab[0, :, base + half:base + rot] = cos_v
        tab[1, :, base:base + half] = -sin_v
        tab[2, :, base + half:base + rot] = sin_v
    return tab


def make_kernel(n_layers, n_z, side, docs, seq_len, d_model, n_heads, ff):
    head_dim = d_model // n_heads
    half_rot = head_dim // 8
    tokens = docs * seq_len
    lanes = 2 * head_dim
    wide_rows = d_model // (2 * n_z)
    down_rows = ff // (2 * n_z)
    n_qkv = 3 * d_model
    n_up0 = ff // 2
    far = n_z // 2

    stages = (
        ("w", 0, n_qkv, 0, wide_rows),
        ("w", n_qkv, d_model + n_up0, 0, wide_rows),
        ("w", n_qkv + d_model + n_up0, ff - n_up0, 0, wide_rows),
        ("d", 0, d_model, 0, down_rows // 2),
        ("d", 0, d_model, down_rows // 2, down_rows // 2),
    )
    per_layer = len(stages)

    def kernel(x_hbm, lens_ref, par_ref, rope_ref, wq_hbm, wo_hbm, wu_hbm, wd_hbm,
               out_hbm, gw, gd,
               x_s, a_s, m_s, q_s, k_s, v_s, ctx_s, act_a, act_b, acc_s,
               w_a, w_b, w_c, w_d0, w_d1, st_q, st_o, st_u, st_d,
               pg, tab, tab_up,
               z_send, c_send, d_send, z_recv, x_recv, y_recv, d_recv,
               p_zsend, p_dsend, p_zrecv, p_drecv,
               x_sem, st_sem, own_sem, ld_sem, out_sem):
        dp = lax.axis_index("dp")
        fs = lax.axis_index("fsdp")
        z, core = lax.div(fs, 2), lax.rem(fs, 2)
        gx, gy = lax.div(dp, side), lax.rem(dp, side)
        par = lax.rem(gx + gy, 2)
        up_z = (dp, lax.rem(z + 1, n_z) * 2 + core)
        dn_z = (dp, lax.rem(z + n_z - 1, n_z) * 2 + core)
        x_dev = (dp + side * (1 - 2 * lax.rem(gx, 2)), fs)
        y_dev = (dp + 1 - 2 * lax.rem(gy, 2), fs)
        sib = (dp, z * 2 + 1 - core)

        def remote(src, dst, send, recv, dev):
            return pltpu.make_async_remote_copy(src_ref=src, dst_ref=dst, send_sem=send, recv_sem=recv,
                                                device_id=dev, device_id_type=MESH)

        def spec_of(s):
            return s // per_layer, stages[s % per_layer]

        def view(s, zz, r0, nr):
            layer, (arr, c0, nc, row0, _) = spec_of(s)
            if arr == "w":
                return gw.at[layer, zz, core, pl.ds(r0, nr), pl.ds(c0, nc)]
            return gd.at[layer, zz, core, pl.ds(row0 + r0, nr), :]

        def own_pieces(s, r0, nr):
            layer, (arr, c0, nc, row0, _) = spec_of(s)
            if arr == "d":
                return [(wd_hbm.at[layer, pl.ds(row0 + r0, nr), :], view(s, z, r0, nr))]
            k = s % per_layer
            if k == 0:
                parts = [(wq_hbm, 0, n_qkv)]
            elif k == 1:
                parts = [(wo_hbm, 0, d_model), (wu_hbm, 0, n_up0)]
            else:
                parts = [(wu_hbm, n_up0, ff - n_up0)]
            out, at = [], c0
            for ref, s0, ns in parts:
                out.append((ref.at[layer, pl.ds(r0, nr), pl.ds(s0, ns)],
                            gw.at[layer, z, core, pl.ds(r0, nr), pl.ds(at, ns)]))
                at += ns
            return out

        def geometry(s):
            rows = spec_of(s)[1][4]
            half, quarter = rows // 2, rows // 4
            mine = pl.multiple_of(par * half, 16)
            other = pl.multiple_of((1 - par) * half, 16)
            return rows, half, quarter, mine, other

        def own_sends(s):
            rows, half, _, mine, _ = geometry(s)
            for src, dst in own_pieces(s, mine, half):
                remote(src, dst, z_send.at[s], z_recv.at[s, 0, 0], up_z).start()
                remote(src, dst, z_send.at[s], z_recv.at[s, 1, 0], dn_z).start()
            for src, dst in own_pieces(s, 0, rows):
                remote(src, dst, d_send.at[s], d_recv.at[s], sib).start()

        def around(d):
            return lax.rem(z - d + n_z, n_z), lax.rem(z + d, n_z)

        def z_tick(s, d):
            _, half, quarter, mine, _ = geometry(s)
            second = pl.multiple_of(mine + quarter, 16)
            lo, hi = around(d)

            @pl.when(d < far)
            def _():
                v_lo, v_hi = view(s, lo, mine, half), view(s, hi, mine, half)
                remote(v_lo, v_lo, z_send.at[s], z_recv.at[s, 0, d - 1], up_z).wait_recv()
                remote(v_hi, v_hi, z_send.at[s], z_recv.at[s, 1, d - 1], dn_z).wait_recv()

                @pl.when(d < far - 1)
                def _():
                    remote(v_lo, v_lo, z_send.at[s], z_recv.at[s, 0, d], up_z).start()
                    remote(v_hi, v_hi, z_send.at[s], z_recv.at[s, 1, d], dn_z).start()

                @pl.when(d == far - 1)
                def _():
                    q_lo, q_hi = view(s, lo, mine, quarter), view(s, hi, second, quarter)
                    remote(q_lo, q_lo, z_send.at[s], z_recv.at[s, 0, d], up_z).start()
                    remote(q_hi, q_hi, z_send.at[s], z_recv.at[s, 1, d], dn_z).start()

                for j, zz in ((0, lo), (1, hi)):
                    c_x, c_y = view(s, zz, mine, quarter), view(s, zz, second, quarter)
                    remote(c_x, c_x, c_send.at[s], x_recv.at[s, j, d - 1], x_dev).start()
                    remote(c_y, c_y, c_send.at[s], y_recv.at[s, j, d - 1], y_dev).start()

            @pl.when(d == far)
            def _():
                c_x, c_y = view(s, lo, mine, quarter), view(s, lo, second, quarter)
                remote(c_x, c_x, z_send.at[s], z_recv.at[s, 0, d - 1], up_z).wait_recv()
                remote(c_y, c_y, z_send.at[s], z_recv.at[s, 1, d - 1], dn_z).wait_recv()
                remote(c_x, c_x, c_send.at[s], x_recv.at[s, 0, d - 1], x_dev).start()
                remote(c_y, c_y, c_send.at[s], y_recv.at[s, 0, d - 1], y_dev).start()

        def d_tick(s, d):
            rows, _, quarter, _, other = geometry(s)
            second = pl.multiple_of(other + quarter, 16)
            lo, hi = around(d)

            def one(zz, j):
                c_x, c_y = view(s, zz, other, quarter), view(s, zz, second, quarter)
                remote(c_x, c_x, c_send.at[s], x_recv.at[s, j, d - 1], x_dev).wait_recv()
                remote(c_y, c_y, c_send.at[s], y_recv.at[s, j, d - 1], y_dev).wait_recv()
                whole = view(s, zz, 0, rows)
                remote(whole, whole, d_send.at[s], d_recv.at[s], sib).start()

            one(lo, 0)

            @pl.when(d < far)
            def _():
                one(hi, 1)

        def all_blocks(s, which):
            layer, (arr, c0, nc, row0, rows) = spec_of(s)
            if arr == "w":
                return gw.at[layer, :, which, :, pl.ds(c0, nc)]
            return gd.at[layer, :, which, pl.ds(row0, rows), :]

        def load_copies(s):
            layer = s // per_layer
            k = s % per_layer
            out = []
            for i in range(STEPS):
                if k == 0:
                    pairs = [(gw.at[layer, :, :, :, pl.ds(i * 3 * TILE, 3 * TILE)], w_a.at[i])]
                elif k == 1:
                    pairs = [(gw.at[layer, :, :, :, pl.ds(n_qkv + i * TILE, TILE)],
                              w_b.at[i, :, :, :, pl.ds(0, TILE)]),
                             (gw.at[layer, :, :, :, pl.ds(n_qkv + d_model + i * 2 * TILE, 2 * TILE)],
                              w_b.at[i, :, :, :, pl.ds(TILE, 2 * TILE)])]
                elif k == 2:
                    pairs = [(gw.at[layer, :, :, :, pl.ds(n_qkv + d_model + n_up0 + i * 2 * TILE, 2 * TILE)], w_c.at[i])]
                else:
                    dst = w_d0 if k == 3 else w_d1
                    pairs = [(gd.at[layer, :, :, pl.ds((k - 3) * (down_rows // 2), down_rows // 2),
                                    pl.ds(i * TILE, TILE)], dst.at[i])]
                out.append([pltpu.make_async_copy(a, b, ld_sem.at[k, i, j]) for j, (a, b) in enumerate(pairs)])
            return out

        def fetch(s):
            sibs = all_blocks(s, 1 - core)
            remote(sibs, sibs, d_send.at[s], d_recv.at[s], sib).wait_recv()
            for cps in load_copies(s):
                for cp in cps:
                    cp.start()

        def wait_load(s, i):
            k = s % per_layer
            bufs = {0: [w_a.at[i]], 1: [w_b.at[i, :, :, :, pl.ds(0, TILE)], w_b.at[i, :, :, :, pl.ds(TILE, 2 * TILE)]],
                    2: [w_c.at[i]], 3: [w_d0.at[i]], 4: [w_d1.at[i]]}[k]
            for j, buf in enumerate(bufs):
                pltpu.make_async_copy(buf, buf, ld_sem.at[k, i, j]).wait()

        x_copy = pltpu.make_async_copy(x_hbm, x_s, x_sem)
        x_copy.start()
        st = [pltpu.make_async_copy(src, dst, st_sem.at[j]) for j, (src, dst) in
              enumerate(((wq_hbm, st_q), (wo_hbm, st_o), (wu_hbm, st_u), (wd_hbm, st_d)))]
        for cp in st:
            cp.start()
        barrier = pltpu.get_barrier_semaphore()
        for dev in (up_z, dn_z, x_dev, y_dev, sib):
            pl.semaphore_signal(barrier, inc=1, device_id=dev, device_id_type=MESH)
        pl.semaphore_wait(barrier, 5)

        remote(par_ref, pg.at[z, core], p_zsend, p_zrecv.at[0, 0], up_z).start()
        remote(par_ref, pg.at[z, core], p_zsend, p_zrecv.at[1, 0], dn_z).start()
        remote(par_ref, pg.at[z, core], p_dsend, p_drecv, sib).start()
        own_sends(0)
        own_sends(1)
        pg[z, core] = par_ref[...]
        for cp in st:
            cp.wait()
        own = []
        for j, (src, c0) in enumerate(((st_q, 0), (st_o, n_qkv), (st_u, n_qkv + d_model))):
            own.append(pltpu.make_async_copy(src, gw.at[:, z, core, :, pl.ds(c0, src.shape[2])], own_sem.at[j]))
        own.append(pltpu.make_async_copy(st_d, gd.at[:, z, core], own_sem.at[3]))
        for cp in own:
            cp.start()

        def p_tick(d):
            lo, hi = around(d)
            v_lo, v_hi = pg.at[lo, core], pg.at[hi, core]
            remote(v_lo, v_lo, p_zsend, p_zrecv.at[0, d - 1], up_z).wait_recv()

            @pl.when(d < far)
            def _():
                remote(v_lo, v_lo, p_zsend, p_zrecv.at[0, d], up_z).start()
                remote(v_hi, v_hi, p_zsend, p_zrecv.at[1, d - 1], dn_z).wait_recv()

            @pl.when(d < far - 1)
            def _():
                remote(v_hi, v_hi, p_zsend, p_zrecv.at[1, d], dn_z).start()

            remote(v_lo, v_lo, p_dsend, p_drecv, sib).start()

            @pl.when(d < far)
            def _():
                remote(v_hi, v_hi, p_dsend, p_drecv, sib).start()

        @pl.loop(0, far)
        def _(i):
            p_tick(i + 1)
            z_tick(0, i + 1)

            @pl.when(i > 0)
            def _():
                d_tick(0, i)

        d_tick(0, far)

        p_all = pg.at[:, 1 - core]
        remote(p_all, p_all, p_dsend, p_drecv, sib).wait_recv()
        low = lax.broadcasted_iota(jnp.int32, (n_layers * PAR_ROWS, lanes), 1) < head_dim
        for zz in range(n_z):
            tab[:, zz * lanes:(zz + 1) * lanes] = jnp.where(low, pg[zz, 0], pg[zz, 1])
            for cc in range(2):
                at = (zz * 2 + cc) * down_rows
                for layer in range(n_layers):
                    for j in range(down_rows // lanes):
                        r = layer * PAR_ROWS + 9 + j
                        tab_up[layer:layer + 1, at + j * lanes:at + (j + 1) * lanes] = pg[zz, cc, r:r + 1, :]
        for cp in own:
            cp.wait()

        def param(layer, j, cols=None):
            r = layer * PAR_ROWS + j
            return tab[r:r + 1, :] if cols is None else tab[r:r + 1, cols]

        def norms(layer):
            @pl.loop(0, tokens // 64)
            def _(t):
                rows = pl.ds(pl.multiple_of(t * 64, 64), 64)
                xf = x_s[rows, :].astype(F32)
                mean = jnp.mean(xf, axis=-1, keepdims=True)
                cen = xf - mean
                var = jnp.mean(cen * cen, axis=-1, keepdims=True)
                nrm = cen * lax.rsqrt(var + LN_EPS)
                a_s[rows, :] = (nrm * param(layer, 0) + param(layer, 1)).astype(BF)
                m_s[rows, :] = (nrm * param(layer, 2) + param(layer, 3)).astype(BF)

        def dot(a, b):
            return jnp.dot(a, b, preferred_element_type=F32)

        def flat(ref, i):
            w = ref[i]
            return w.reshape(w.shape[0] * w.shape[1] * w.shape[2], w.shape[3])

        def rope(u):
            out = []
            for r0 in range(0, u.shape[0], seq_len):
                row = []
                for c0 in range(0, u.shape[1], lanes):
                    v = u[r0:r0 + seq_len, c0:c0 + lanes].astype(F32)
                    row.append((v * rope_ref[0] + pltpu.roll(v, lanes - half_rot, 1) * rope_ref[1]
                                + pltpu.roll(v, half_rot, 1) * rope_ref[2]).astype(BF))
                out.append(jnp.concatenate(row, axis=1))
            return jnp.concatenate(out, axis=0)

        def row_loop(block, body):
            @pl.loop(0, tokens // block)
            def _(t):
                body(pl.ds(pl.multiple_of(t * block, block), block))

        def qkv_step(layer, i):
            w = flat(w_a, i)
            cols = pl.ds(pl.multiple_of(i * TILE, TILE), TILE)

            def body(rows):
                r = dot(a_s[rows, :], w)
                q = (r[:, :TILE] + param(layer, 4, cols)).astype(BF)
                k = (r[:, TILE:2 * TILE] + param(layer, 5, cols)).astype(BF)
                q_s[rows, cols] = rope(q)
                k_s[rows, cols] = rope(k)
                v_s[rows, cols] = (r[:, 2 * TILE:] + param(layer, 6, cols)).astype(BF)

            row_loop(256, body)

        def attend(n):
            rows = pl.ds(pl.multiple_of(n * seq_len, seq_len), seq_len)
            pos_q = lax.broadcasted_iota(jnp.int32, (seq_len, seq_len), 0)
            pos_k = lax.broadcasted_iota(jnp.int32, (seq_len, seq_len), 1)
            vis = pos_k <= jnp.minimum(pos_q, lens_ref[n] - 1)
            first = lax.broadcasted_iota(jnp.int32, (seq_len, lanes), 1) < head_dim
            zero = jnp.zeros((seq_len, lanes), BF)

            for p in range(n_heads // 2):
                cs = slice(p * lanes, (p + 1) * lanes)
                q2, k2, v2 = q_s[rows, cs], k_s[rows, cs], v_s[rows, cs]
                kk = jnp.concatenate([jnp.where(first, k2, zero), jnp.where(first, zero, k2)], axis=0)
                vv = jnp.concatenate([jnp.where(first, v2, zero), jnp.where(first, zero, v2)], axis=0)
                sc = lax.dot_general(q2, kk, (((1,), (1,)), ((), ())), preferred_element_type=F32)
                probs = []
                for j in range(2):
                    s1 = jnp.where(vis, sc[:, j * seq_len:(j + 1) * seq_len] * (head_dim ** -0.5), -1e30)
                    e = jnp.exp(s1 - jnp.max(s1, axis=-1, keepdims=True))
                    probs.append((e * (1.0 / jnp.sum(e, axis=-1, keepdims=True))).astype(BF))
                ctx_s[rows, cs] = dot(jnp.concatenate(probs, axis=1), vv).astype(BF)

        def gelu_store(layer, u, rows, first_col, i, base):
            u = u + tab_up[layer:layer + 1, pl.ds(pl.multiple_of(first_col + i * 2 * TILE, 2 * TILE), 2 * TILE)]
            g = (u * 0.5 * (1.0 + lax.erf(u * (2.0 ** -0.5)))).astype(BF)
            cols = pl.ds(pl.multiple_of(base + i * TILE, TILE), TILE)
            act_a[rows, cols] = jnp.concatenate([g[:, :lanes], g[:, 2 * lanes:3 * lanes]], axis=1)
            act_b[rows, cols] = jnp.concatenate([g[:, lanes:2 * lanes], g[:, 3 * lanes:]], axis=1)

        def out_up_step(layer, i):
            w = flat(w_b, i)
            cols = pl.ds(pl.multiple_of(i * TILE, TILE), TILE)

            def body(rows):
                o = dot(ctx_s[rows, :], w[:, :TILE]) + param(layer, 7, cols)
                acc_s[rows, cols] = x_s[rows, cols].astype(F32) + o
                gelu_store(layer, dot(m_s[rows, :], w[:, TILE:]), rows, 0, i, 0)

            row_loop(256, body)

        def up_step(layer, i):
            w = flat(w_c, i)

            def body(rows):
                gelu_store(layer, dot(m_s[rows, :], w), rows, n_up0, i, n_up0 // 2)

            row_loop(256, body)

        def down0_step(layer, i):
            w = flat(w_d0, i)
            cols = pl.ds(pl.multiple_of(i * TILE, TILE), TILE)

            def body(rows):
                acc_s[rows, cols] += dot(act_a[rows, :], w)

            row_loop(256, body)

        def down1_step(layer, i):
            w = flat(w_d1, i)
            cols = pl.ds(pl.multiple_of(i * TILE, TILE), TILE)

            def body(rows):
                y = acc_s[rows, cols] + (dot(act_b[rows, :], w) + param(layer, 8, cols))
                x_s[rows, cols] = y.astype(BF)

            row_loop(256, body)

        def full_ticks(s, i):
            z_tick(s, i + 1)

            @pl.when(i > 0)
            def _():
                d_tick(s, i)

        def half_ticks(s, i, d0):
            d = d0 + lax.div(i, 2)

            @pl.when(lax.rem(i, 2) == 0)
            def _():
                z_tick(s, d)

            @pl.when(lax.rem(i, 2) == 1)
            def _():
                d_tick(s, d)

        x_copy.wait()
        norms(0)
        fetch(0)
        own_sends(2)

        for layer in range(n_layers):
            s0 = layer * per_layer
            more = layer + 1 < n_layers

            @pl.loop(0, STEPS)
            def _(i):
                half_ticks(s0 + 1, i, 1)
                wait_load(s0, i)
                qkv_step(layer, i)

            @pl.loop(0, docs // 2)
            def _(i):
                half_ticks(s0 + 1, i, 3)
                attend(i)

            own_sends(s0 + 3)

            @pl.loop(0, docs // 2)
            def _(i):
                full_ticks(s0 + 2, i)

                @pl.when(i == 2)
                def _():
                    fetch(s0 + 1)

                attend(i + docs // 2)

            d_tick(s0 + 2, far)
            own_sends(s0 + 4)

            @pl.loop(0, STEPS)
            def _(i):
                full_ticks(s0 + 3, i)

                @pl.when(i == 2)
                def _():
                    fetch(s0 + 2)

                wait_load(s0 + 1, i)
                out_up_step(layer, i)

            d_tick(s0 + 3, far)
            if more:
                own_sends(s0 + 5)

            @pl.loop(0, STEPS)
            def _(i):
                full_ticks(s0 + 4, i)

                @pl.when(i == 2)
                def _():
                    fetch(s0 + 3)

                wait_load(s0 + 2, i)
                up_step(layer, i)

            d_tick(s0 + 4, far)
            if more:
                own_sends(s0 + 6)

            @pl.loop(0, STEPS)
            def _(i):
                if more:
                    half_ticks(s0 + 5, i, 1)

                @pl.when(i == 2)
                def _():
                    fetch(s0 + 4)

                wait_load(s0 + 3, i)
                down0_step(layer, i)

            @pl.loop(0, STEPS)
            def _(i):
                if more:
                    half_ticks(s0 + 5, i, 3)
                wait_load(s0 + 4, i)
                down1_step(layer, i)
                if not more:
                    cols = pl.ds(pl.multiple_of(i * TILE, TILE), TILE)
                    pltpu.make_async_copy(x_s.at[:, cols], out_hbm.at[:, cols], out_sem.at[i]).start()

            if more:
                norms(layer + 1)
                fetch(s0 + 5)
                own_sends(s0 + 7)

        for s in range(n_layers * per_layer):
            layer, (arr, c0, nc, row0, rows) = spec_of(s)
            half = rows // 2
            if arr == "w":
                sevenths = gw.at[layer, pl.ds(0, n_z - 1), 0, pl.ds(0, half), pl.ds(c0, nc)]
            else:
                sevenths = gd.at[layer, pl.ds(0, n_z - 1), 0, pl.ds(row0, half), :]
            remote(sevenths, sevenths, z_send.at[s], z_recv.at[s, 0, 0], up_z).wait_send()
            remote(sevenths, sevenths, c_send.at[s], z_recv.at[s, 0, 0], up_z).wait_send()
            every = all_blocks(s, 0)
            remote(every, every, d_send.at[s], d_recv.at[s], sib).wait_send()
        seven = pg.at[pl.ds(0, n_z - 1), 0]
        remote(seven, seven, p_zsend, p_drecv, up_z).wait_send()
        eight = pg.at[:, 0]
        remote(eight, eight, p_dsend, p_drecv, sib).wait_send()
        for i in range(STEPS):
            cols = pl.ds(i * TILE, TILE)
            pltpu.make_async_copy(x_s.at[:, cols], out_hbm.at[:, cols], out_sem.at[i]).wait()

    n_st = n_layers * per_layer
    wide = n_qkv + d_model + ff
    out_shape = (
        jax.ShapeDtypeStruct((tokens, d_model), BF),
        jax.ShapeDtypeStruct((n_layers, n_z, 2, wide_rows, wide), BF),
        jax.ShapeDtypeStruct((n_layers, n_z, 2, down_rows, d_model), BF),
    )
    dma = pltpu.SemaphoreType.DMA
    scratch = [
        pltpu.VMEM((tokens, d_model), BF), pltpu.VMEM((tokens, d_model), BF), pltpu.VMEM((tokens, d_model), BF),
        pltpu.VMEM((tokens, d_model), BF), pltpu.VMEM((tokens, d_model), BF), pltpu.VMEM((tokens, d_model), BF),
        pltpu.VMEM((tokens, d_model), BF),
        pltpu.VMEM((tokens, ff // 2), BF), pltpu.VMEM((tokens, ff // 2), BF), pltpu.VMEM((tokens, d_model), F32),
        pltpu.VMEM((STEPS, n_z, 2, wide_rows, 3 * TILE), BF), pltpu.VMEM((STEPS, n_z, 2, wide_rows, 3 * TILE), BF),
        pltpu.VMEM((STEPS, n_z, 2, wide_rows, 2 * TILE), BF),
        pltpu.VMEM((STEPS, n_z, 2, down_rows // 2, TILE), BF), pltpu.VMEM((STEPS, n_z, 2, down_rows // 2, TILE), BF),
        pltpu.VMEM((n_layers, wide_rows, n_qkv), BF), pltpu.VMEM((n_layers, wide_rows, d_model), BF),
        pltpu.VMEM((n_layers, wide_rows, ff), BF), pltpu.VMEM((n_layers, down_rows, d_model), BF),
        pltpu.VMEM((n_z, 2, n_layers * PAR_ROWS, lanes), F32),
        pltpu.VMEM((n_layers * PAR_ROWS, d_model), F32), pltpu.VMEM((8, ff), F32),
        dma((n_st,)), dma((n_st,)), dma((n_st,)),
        dma((n_st, 2, far)), dma((n_st, 2, far)), dma((n_st, 2, far)), dma((n_st,)),
        dma(()), dma(()), dma((2, far)), dma(()),
        dma(()), dma((4,)), dma((4,)), dma((per_layer, STEPS, 2)), dma((STEPS,)),
    ]
    hbm = pl.BlockSpec(memory_space=pltpu.HBM)
    vmem = pl.BlockSpec(memory_space=pltpu.VMEM)
    smem = pl.BlockSpec(memory_space=pltpu.SMEM)
    return pl.pallas_call(
        kernel,
        name="layers",
        out_shape=out_shape,
        in_specs=[hbm, smem, vmem, vmem, hbm, hbm, hbm, hbm],
        out_specs=(hbm, hbm, hbm),
        scratch_shapes=scratch,
        compiler_params=pltpu.CompilerParams(collective_id=0, has_side_effects=True, vmem_limit_bytes=67043328),
    )


def solution(mesh):
    row_spec = P(('dp', 'fsdp'), None, None)
    in_specs = (row_spec, P(('dp', 'fsdp')), P(None, None, 'fsdp'), P(None, 'fsdp', None, None), P(None, 'fsdp'), P(None, 'fsdp', None), P(None, 'fsdp'), P(None, 'fsdp', None), P(None, 'fsdp'), P(None, 'fsdp', None), P(None, 'fsdp'))
    n_z = mesh.shape['fsdp'] // 2
    side = math.isqrt(mesh.shape['dp'])

    def local_step(hidden, lens, ln_par, w_qkv, b_qkv, w_out, b_out, w_up, b_up, w_down, b_down):
        docs, seq_len, d_model = hidden.shape
        n_layers, rows, n_heads, triple = w_qkv.shape
        head_dim = triple // 3
        ff = w_up.shape[2]
        per_tile = TILE // head_dim
        wq = w_qkv.reshape(n_layers, rows, n_heads // per_tile, per_tile, 3, head_dim)
        wq = wq.transpose(0, 1, 2, 4, 3, 5).reshape(n_layers, rows, 3 * d_model)
        small = jnp.concatenate([ln_par, b_qkv.astype(F32).reshape(n_layers, 3, -1), b_out.astype(F32)[:, None],
                                 b_down.astype(F32)[:, None]], axis=1)
        small = jnp.concatenate([small, small], axis=2)
        small = jnp.concatenate([small, b_up.astype(F32).reshape(n_layers, -1, 2 * head_dim)], axis=1)
        small = jnp.pad(small, ((0, 0), (0, PAR_ROWS - small.shape[1]), (0, 0))).reshape(-1, 2 * head_dim)
        rope = jnp.asarray(rotary_lanes(seq_len, head_dim))
        call = make_kernel(n_layers, n_z, side, docs, seq_len, d_model, n_heads, ff)
        out = call(hidden.reshape(docs * seq_len, d_model), lens, small, rope, wq, w_out, w_up, w_down)[0]
        return out.reshape(docs, seq_len, d_model)

    return jax.shard_map(local_step, mesh=mesh, in_specs=in_specs, out_specs=row_spec, check_vma=False)
```

```python
import math

import jax
import jax.numpy as jnp
import numpy as np
from jax import lax
from jax.experimental import pallas as pl
from jax.experimental.pallas import tpu as pltpu
from jax.sharding import PartitionSpec as P

MESH = pl.DeviceIdType.MESH
ROPE_BASE = 10000.0
LN_EPS = 1e-5
BF = jnp.bfloat16
F32 = jnp.float32
TILE = 256
BLOCKS = 4
PAR_ROWS = 16


def rotary_lanes(seq_len, head_dim):
    rot = head_dim // 4
    half = rot // 2
    inv_freq = (1.0 / (ROPE_BASE ** (np.arange(0, rot, 2, dtype=np.float32) / rot))).astype(np.float32)
    angles = np.arange(seq_len, dtype=np.float32)[:, None] * inv_freq[None, :]
    cos_v, sin_v = np.cos(angles), np.sin(angles)
    tab = np.zeros((3, seq_len, 2 * head_dim), np.float32)
    tab[0] = 1.0
    for base in (0, head_dim):
        tab[0, :, base:base + half] = cos_v
        tab[0, :, base + half:base + rot] = cos_v
        tab[1, :, base:base + half] = -sin_v
        tab[2, :, base + half:base + rot] = sin_v
    return tab


def make_kernel(n_layers, n_z, side, docs, seq_len, d_model, n_heads, ff):
    head_dim = d_model // n_heads
    half_rot = head_dim // 8
    tokens = docs * seq_len
    lanes = 2 * head_dim
    rows_w = d_model // (2 * n_z)
    down_rows = ff // (2 * n_z)
    n_up = ff // d_model
    far = n_z // 2
    half, quarter = rows_w // 2, rows_w // 4
    per_layer = 4 + 2 * n_up
    n_st = n_layers * per_layer
    d_cols = d_model // n_up
    parts = down_rows // rows_w
    blk = tokens // BLOCKS

    def kernel(x_hbm, lens_ref, par_ref, rope_ref, wq_hbm, wo_hbm, wu_hbm, wd_hbm,
               out_hbm, g,
               x_s, a_s, m_s, qkv_s, ctx_s, act_s, acc_s, w_s, wd_s, st_q, st_o, st_u, st_d,
               pg, tab, tab_up,
               z_send, c_send, d_send, z_recv, x_recv, y_recv, d_recv,
               p_zsend, p_dsend, p_zrecv, p_drecv,
               x_sem, st_sem, own_sem, ld_sem, ldd_sem, out_sem):
        dp = lax.axis_index("dp")
        fs = lax.axis_index("fsdp")
        z, core = lax.div(fs, 2), lax.rem(fs, 2)
        gx, gy = lax.div(dp, side), lax.rem(dp, side)
        par = lax.rem(gx + gy, 2)
        up_z = (dp, lax.rem(z + 1, n_z) * 2 + core)
        dn_z = (dp, lax.rem(z + n_z - 1, n_z) * 2 + core)
        x_dev = (dp + side * (1 - 2 * lax.rem(gx, 2)), fs)
        y_dev = (dp + 1 - 2 * lax.rem(gy, 2), fs)
        sib = (dp, z * 2 + 1 - core)
        mine = pl.multiple_of(par * half, 16)
        mine2 = pl.multiple_of(par * half + quarter, 16)
        other = pl.multiple_of((1 - par) * half, 16)
        other2 = pl.multiple_of((1 - par) * half + quarter, 16)

        def remote(src, dst, send, recv, dev):
            return pltpu.make_async_remote_copy(src_ref=src, dst_ref=dst, send_sem=send, recv_sem=recv,
                                                device_id=dev, device_id_type=MESH)

        def same(ref, send, recv, dev):
            return remote(ref, ref, send, recv, dev)

        def view(s, zz, r0, nr):
            return g.at[s, zz, core, pl.ds(r0, nr), :]

        def around(d):
            return lax.rem(z - d + n_z, n_z), lax.rem(z + d, n_z)

        def guard(s, fn):
            if isinstance(s, int):
                if 0 <= s < n_st:
                    fn()
            else:
                pl.when(s < n_st)(fn)

        def own_send(s, src=None):
            piece = view(s, z, mine, half) if src is None else src(mine, half)
            whole = view(s, z, 0, rows_w) if src is None else src(0, rows_w)
            remote(piece, view(s, z, mine, half), z_send.at[s], z_recv.at[s, 0, 0], up_z).start()
            remote(piece, view(s, z, mine, half), z_send.at[s], z_recv.at[s, 1, 0], dn_z).start()
            remote(whole, view(s, z, 0, rows_w), d_send.at[s], d_recv.at[s], sib).start()

        def z_hop(s, d):
            lo, hi = around(d)
            if d == far:
                c_x, c_y = view(s, lo, mine, quarter), view(s, lo, mine2, quarter)
                same(c_x, z_send.at[s], z_recv.at[s, 0, d - 1], up_z).wait_recv()
                same(c_x, c_send.at[s], x_recv.at[s, 0, d - 1], x_dev).start()
                same(c_y, z_send.at[s], z_recv.at[s, 1, d - 1], dn_z).wait_recv()
                same(c_y, c_send.at[s], y_recv.at[s, 0, d - 1], y_dev).start()
                return
            for j, zz, nxt in ((0, lo, up_z), (1, hi, dn_z)):
                v = view(s, zz, mine, half)
                same(v, z_send.at[s], z_recv.at[s, j, d - 1], nxt).wait_recv()
                if d == far - 1:
                    v = view(s, zz, (mine, mine2)[j], quarter)
                same(v, z_send.at[s], z_recv.at[s, j, d], nxt).start()
                c_x, c_y = view(s, zz, mine, quarter), view(s, zz, mine2, quarter)
                same(c_x, c_send.at[s], x_recv.at[s, j, d - 1], x_dev).start()
                same(c_y, c_send.at[s], y_recv.at[s, j, d - 1], y_dev).start()

        def d_hop(s, d):
            for j, zz in enumerate(around(d)[:1 if d == far else 2]):
                c_x, c_y = view(s, zz, other, quarter), view(s, zz, other2, quarter)
                same(c_x, c_send.at[s], x_recv.at[s, j, d - 1], x_dev).wait_recv()
                same(c_y, c_send.at[s], y_recv.at[s, j, d - 1], y_dev).wait_recv()
                same(view(s, zz, 0, rows_w), d_send.at[s], d_recv.at[s], sib).start()

        def tick_z(t):
            for d in range(far, 0, -1):
                guard(t - d + 1, lambda d=d: z_hop(t - d + 1, d))
            guard(t + 2, lambda: own_send(t + 2))

        def tick_d(t):
            for d in range(far, 0, -1):
                guard(t - d, lambda d=d: d_hop(t - d, d))

        def loads(s, slot, down):
            if not down:
                return [pltpu.make_async_copy(g.at[s], w_s.at[slot], ld_sem.at[slot])]
            return [pltpu.make_async_copy(g.at[s, :, :, :, pl.ds(q * d_cols, d_cols)],
                                          wd_s.at[slot, :, :, pl.ds(q * rows_w, rows_w), :], ldd_sem.at[slot, q])
                    for q in range(parts)]

        def fetch(s, slot, down=False):
            sibs = g.at[s, :, 1 - core]
            same(sibs, d_send.at[s], d_recv.at[s], sib).wait_recv()
            for cp in loads(s, slot, down):
                cp.start()

        x_copy = pltpu.make_async_copy(x_hbm, x_s, x_sem)
        st = [pltpu.make_async_copy(src, dst, st_sem.at[j]) for j, (src, dst) in
              enumerate(((wq_hbm, st_q), (wo_hbm, st_o), (wu_hbm, st_u), (wd_hbm, st_d)))]
        for cp in st:
            cp.start()
        x_copy.start()
        barrier = pltpu.get_barrier_semaphore()
        for dev in (up_z, dn_z, x_dev, y_dev, sib):
            pl.semaphore_signal(barrier, inc=1, device_id=dev, device_id_type=MESH)
        pl.semaphore_wait(barrier, 5)

        remote(par_ref, pg.at[z, core], p_zsend, p_zrecv.at[0, 0], up_z).start()
        remote(par_ref, pg.at[z, core], p_zsend, p_zrecv.at[1, 0], dn_z).start()
        remote(par_ref, pg.at[z, core], p_dsend, p_drecv, sib).start()
        for s in range(2):
            own_send(s, lambda r0, nr, s=s: wq_hbm.at[0, pl.ds(r0, nr), pl.ds(s * d_model, d_model)])
        pg[z, core] = par_ref[...]
        for cp in st:
            cp.wait()
        own = []
        for layer in range(n_layers):
            pieces = [(0, st_q.at[layer, :, pl.ds(j * d_model, d_model)], j) for j in range(3)]
            pieces.append((0, st_o.at[layer], 3))
            pieces += [(0, st_u.at[layer, :, pl.ds(j * d_model, d_model)], 4 + j) for j in range(n_up)]
            for j in range(n_up):
                for q in range(parts):
                    pieces.append((q, st_d.at[layer, pl.ds(q * rows_w, rows_w), pl.ds(j * d_cols, d_cols)], 4 + n_up + j))
            for q, src, j in pieces:
                dst = g.at[layer * per_layer + j, z, core]
                if j >= 4 + n_up:
                    dst = g.at[layer * per_layer + j, z, core, :, pl.ds(q * d_cols, d_cols)]
                own.append(pltpu.make_async_copy(src, dst, own_sem.at[len(own)]))
        for cp in own:
            cp.start()
        for cp in own:
            cp.wait()

        def p_hop(d):
            lo, hi = around(d)
            v_lo, v_hi = pg.at[lo, core], pg.at[hi, core]
            same(v_lo, p_zsend, p_zrecv.at[0, d - 1], up_z).wait_recv()
            if d < far:
                same(v_lo, p_zsend, p_zrecv.at[0, d], up_z).start()
                same(v_hi, p_zsend, p_zrecv.at[1, d - 1], dn_z).wait_recv()
            if d < far - 1:
                same(v_hi, p_zsend, p_zrecv.at[1, d], dn_z).start()
            same(v_lo, p_dsend, p_drecv, sib).start()
            if d < far:
                same(v_hi, p_dsend, p_drecv, sib).start()

        for t in range(far):
            p_hop(t + 1)
            tick_z(t)
            tick_d(t)
        tick_z(far)
        tick_d(far)

        p_all = pg.at[:, 1 - core]
        same(p_all, p_dsend, p_drecv, sib).wait_recv()
        low = lax.broadcasted_iota(jnp.int32, (PAR_ROWS, lanes), 1) < head_dim
        for layer in range(n_layers):
            r0 = layer * PAR_ROWS
            for zz in range(n_z):
                tab[layer, :, zz * lanes:(zz + 1) * lanes] = jnp.where(
                    low, pg[zz, 0, r0:r0 + PAR_ROWS, :], pg[zz, 1, r0:r0 + PAR_ROWS, :])
                for cc in range(2):
                    at = (zz * 2 + cc) * down_rows
                    for j in range(down_rows // lanes):
                        r = r0 + 9 + j
                        tab_up[layer, 0:1, at + j * lanes:at + (j + 1) * lanes] = pg[zz, cc, r:r + 1, :]
            for b in range(3 * n_z):
                two = []
                for p in (2 * b, 2 * b + 1):
                    dev, r = p // 3, r0 + 4 + p % 3
                    two.append(pg[dev // 2, dev % 2, r:r + 1, :])
                c0 = (b % n_z) * lanes
                tab[layer, 4 + b // n_z:5 + b // n_z, c0:c0 + lanes] = jnp.where(low[0:1], two[0], two[1])

        def norms(layer):
            @pl.loop(0, tokens // 64)
            def _(t):
                rows = pl.ds(pl.multiple_of(t * 64, 64), 64)
                xf = x_s[rows, :].astype(F32)
                mean = jnp.mean(xf, axis=-1, keepdims=True)
                cen = xf - mean
                var = jnp.mean(cen * cen, axis=-1, keepdims=True)
                nrm = cen * lax.rsqrt(var + LN_EPS)
                a_s[rows, :] = (nrm * tab[layer, 0:1, :] + tab[layer, 1:2, :]).astype(BF)
                m_s[rows, :] = (nrm * tab[layer, 2:3, :] + tab[layer, 3:4, :]).astype(BF)

        def dot(a, b):
            return jnp.dot(a, b, preferred_element_type=F32)

        def rows_of(r):
            return pl.ds(pl.multiple_of(r * blk, blk), blk)

        def w_tile(slot, c0, nc):
            return w_s[slot, :, :, :, c0:c0 + nc].reshape(d_model, nc)

        def qkv_block(layer, j, slot, r):
            rows = rows_of(r)
            for c0 in range(0, d_model, TILE):
                y = dot(a_s[rows, :], w_tile(slot, c0, TILE)) + tab[layer, pl.ds(4 + j, 1), c0:c0 + TILE]
                qkv_s[j, rows, c0:c0 + TILE] = y.astype(BF)

        def attend(n):
            rows = pl.ds(pl.multiple_of(n * seq_len, seq_len), seq_len)
            pos_q = lax.broadcasted_iota(jnp.int32, (seq_len, seq_len), 0)
            pos_k = lax.broadcasted_iota(jnp.int32, (seq_len, seq_len), 1)
            vis = pos_k <= jnp.minimum(pos_q, lens_ref[n] - 1)
            first = lax.broadcasted_iota(jnp.int32, (seq_len, lanes), 1) < head_dim
            zero = jnp.zeros((seq_len, lanes), BF)

            def rope(v):
                v = v.astype(F32)
                return (v * rope_ref[0] + pltpu.roll(v, lanes - half_rot, 1) * rope_ref[1]
                        + pltpu.roll(v, half_rot, 1) * rope_ref[2]).astype(BF)

            for p in range(n_heads // 2):
                cs = slice(p * lanes, (p + 1) * lanes)
                trio = []
                for b in range(3 * p, 3 * p + 3):
                    trio.append(qkv_s[b // n_z, rows, (b % n_z) * lanes:(b % n_z + 1) * lanes])
                q2 = rope(jnp.where(first, trio[0], trio[1]))
                k2 = rope(pltpu.roll(jnp.where(first, trio[2], trio[0]).astype(F32), head_dim, 1))
                v2 = jnp.where(first, trio[1], trio[2])
                kk = jnp.concatenate([jnp.where(first, k2, zero), jnp.where(first, zero, k2)], axis=0)
                vv = jnp.concatenate([jnp.where(first, v2, zero), jnp.where(first, zero, v2)], axis=0)
                sc = lax.dot_general(q2, kk, (((1,), (1,)), ((), ())), preferred_element_type=F32)
                probs = []
                for j in range(2):
                    s1 = jnp.where(vis, sc[:, j * seq_len:(j + 1) * seq_len] * (head_dim ** -0.5), -1e30)
                    e = jnp.exp(s1 - jnp.max(s1, axis=-1, keepdims=True))
                    probs.append((e * (1.0 / jnp.sum(e, axis=-1, keepdims=True))).astype(BF))
                ctx_s[rows, cs] = dot(jnp.concatenate(probs, axis=1), vv).astype(BF)

        def out_block(layer, slot, r):
            rows = rows_of(r)
            for c0 in range(0, d_model, TILE):
                cols = slice(c0, c0 + TILE)
                o = dot(ctx_s[rows, :], w_tile(slot, c0, TILE)) + tab[layer, 7:8, cols]
                acc_s[rows, cols] = x_s[rows, cols].astype(F32) + o

        def up_block(layer, j, slot, r):
            rows = rows_of(r)
            for c0 in range(0, d_model, TILE):
                cols = pl.ds(pl.multiple_of(j * d_model + c0, TILE), TILE)
                u = dot(m_s[rows, :], w_tile(slot, c0, TILE)) + tab_up[layer, 0:1, cols]
                act_s[rows, cols] = (u * 0.5 * (1.0 + lax.erf(u * (2.0 ** -0.5)))).astype(BF)

        def down_block(layer, j, slot, r):
            rows = rows_of(r)
            cols = pl.ds(pl.multiple_of(j * d_cols, d_cols), d_cols)
            w = wd_s[slot].reshape(ff, d_cols)
            y = acc_s[rows, cols] + (dot(act_s[rows, :], w) + tab[layer, 8:9, cols])
            x_s[rows, cols] = y.astype(BF)

        def out_copy(j):
            cols = pl.ds(pl.multiple_of(j * d_cols, d_cols), d_cols)
            return pltpu.make_async_copy(x_s.at[:, cols], out_hbm.at[:, cols], out_sem.at[j])

        x_copy.wait()
        norms(0)
        fetch(0, 0)

        @pl.loop(0, n_layers)
        def _(layer):
            s0 = layer * per_layer
            t0 = s0 + far + 1

            @pl.loop(0, 3)
            def _(j):
                slot = lax.rem(j, 2)

                @pl.loop(0, BLOCKS)
                def _(r):
                    @pl.when(r == 0)
                    def _():
                        tick_z(t0 + j)
                        loads(s0 + j, slot, False)[0].wait()

                    @pl.when(r == 2)
                    def _():
                        tick_d(t0 + j)

                    qkv_block(layer, j, slot, r)

                    @pl.when(r == BLOCKS - 1)
                    def _():
                        fetch(s0 + j + 1, 1 - slot)

            @pl.loop(0, docs)
            def _(n):
                t = t0 + 3 + lax.div(n, docs // 2)

                @pl.when(lax.rem(n, docs // 2) == 0)
                def _():
                    tick_z(t)

                @pl.when(lax.rem(n, docs // 2) == 2)
                def _():
                    tick_d(t)

                attend(n)

            loads(s0 + 3, 1, False)[0].wait()
            fetch(s0 + 4, 0)

            @pl.loop(0, BLOCKS)
            def _(r):
                out_block(layer, 1, r)

            @pl.loop(0, n_up)
            def _(j):
                slot = lax.rem(j, 2)

                @pl.loop(0, BLOCKS)
                def _(r):
                    @pl.when(r == 0)
                    def _():
                        tick_z(t0 + 5 + j)
                        loads(s0 + 4 + j, slot, False)[0].wait()

                    @pl.when(r == 2)
                    def _():
                        tick_d(t0 + 5 + j)

                    up_block(layer, j, slot, r)

                    @pl.when((r == BLOCKS - 1) & (j < n_up - 1))
                    def _():
                        fetch(s0 + 5 + j, 1 - slot)

                    @pl.when((r == BLOCKS - 1) & (j == n_up - 1))
                    def _():
                        fetch(s0 + 4 + n_up, 0, True)

            @pl.loop(0, n_up)
            def _(j):
                slot = lax.rem(j, 2)

                @pl.loop(0, BLOCKS)
                def _(r):
                    @pl.when((r == 0) & (j < n_up - 1))
                    def _():
                        tick_z(t0 + 5 + n_up + j)

                    @pl.when(r == 0)
                    def _():
                        for cp in loads(s0 + 4 + n_up + j, slot, True):
                            cp.wait()

                    @pl.when((r == 2) & (j < n_up - 1))
                    def _():
                        tick_d(t0 + 5 + n_up + j)

                    down_block(layer, j, slot, r)

                    @pl.when((r == BLOCKS - 1) & (j < n_up - 1))
                    def _():
                        fetch(s0 + 5 + n_up + j, 1 - slot, True)

                    @pl.when((r == BLOCKS - 1) & (j == n_up - 1) & (layer < n_layers - 1))
                    def _():
                        fetch(s0 + per_layer, 0)

                @pl.when(layer == n_layers - 1)
                def _():
                    out_copy(j).start()

            @pl.when(layer < n_layers - 1)
            def _():
                norms(layer + 1)

        @pl.loop(0, n_st)
        def _(s):
            sevenths = g.at[s, pl.ds(0, n_z - 1), 0, pl.ds(0, half), :]
            same(sevenths, z_send.at[s], z_recv.at[s, 0, 0], up_z).wait_send()
            same(sevenths, c_send.at[s], z_recv.at[s, 0, 0], up_z).wait_send()
            same(g.at[s, :, 0], d_send.at[s], d_recv.at[s], sib).wait_send()

        seven = pg.at[pl.ds(0, n_z - 1), 0]
        same(seven, p_zsend, p_drecv, up_z).wait_send()
        eight = pg.at[:, 0]
        same(eight, p_dsend, p_drecv, sib).wait_send()
        for j in range(n_up):
            out_copy(j).wait()

    out_shape = (
        jax.ShapeDtypeStruct((tokens, d_model), BF),
        jax.ShapeDtypeStruct((n_st, n_z, 2, rows_w, d_model), BF),
    )
    dma = pltpu.SemaphoreType.DMA
    n_own = n_layers * (4 + n_up + n_up * parts)
    act = pltpu.VMEM((tokens, d_model), BF)
    scratch = [
        act, act, act, pltpu.VMEM((3, tokens, d_model), BF), act, pltpu.VMEM((tokens, ff), BF),
        pltpu.VMEM((tokens, d_model), F32),
        pltpu.VMEM((2, n_z, 2, rows_w, d_model), BF), pltpu.VMEM((2, n_z, 2, down_rows, d_cols), BF),
        pltpu.VMEM((n_layers, rows_w, 3 * d_model), BF), pltpu.VMEM((n_layers, rows_w, d_model), BF),
        pltpu.VMEM((n_layers, rows_w, ff), BF), pltpu.VMEM((n_layers, down_rows, d_model), BF),
        pltpu.VMEM((n_z, 2, n_layers * PAR_ROWS, lanes), F32),
        pltpu.VMEM((n_layers, PAR_ROWS, d_model), F32), pltpu.VMEM((n_layers, 8, ff), F32),
        dma((n_st,)), dma((n_st,)), dma((n_st,)),
        dma((n_st, 2, far)), dma((n_st, 2, far)), dma((n_st, 2, far)), dma((n_st,)),
        dma(()), dma(()), dma((2, far)), dma(()),
        dma(()), dma((4,)), dma((n_own,)), dma((2,)), dma((2, parts)), dma((n_up,)),
    ]
    hbm = pl.BlockSpec(memory_space=pltpu.HBM)
    vmem = pl.BlockSpec(memory_space=pltpu.VMEM)
    smem = pl.BlockSpec(memory_space=pltpu.SMEM)
    return pl.pallas_call(
        kernel,
        name="layers",
        out_shape=out_shape,
        in_specs=[hbm, smem, vmem, vmem, hbm, hbm, hbm, hbm],
        out_specs=(hbm, hbm),
        scratch_shapes=scratch,
        compiler_params=pltpu.CompilerParams(collective_id=0, has_side_effects=True, vmem_limit_bytes=67043328),
    )


def solution(mesh):
    row_spec = P(('dp', 'fsdp'), None, None)
    in_specs = (row_spec, P(('dp', 'fsdp')), P(None, None, 'fsdp'), P(None, 'fsdp', None, None), P(None, 'fsdp'), P(None, 'fsdp', None), P(None, 'fsdp'), P(None, 'fsdp', None), P(None, 'fsdp'), P(None, 'fsdp', None), P(None, 'fsdp'))
    n_z = mesh.shape['fsdp'] // 2
    side = math.isqrt(mesh.shape['dp'])

    def local_step(hidden, lens, ln_par, w_qkv, b_qkv, w_out, b_out, w_up, b_up, w_down, b_down):
        docs, seq_len, d_model = hidden.shape
        n_layers, rows, n_heads, triple = w_qkv.shape
        head_dim = triple // 3
        ff = w_up.shape[2]
        wq = w_qkv.reshape(n_layers, rows, n_heads * triple)
        small = jnp.concatenate([ln_par, b_qkv.astype(F32).reshape(n_layers, 3, -1), b_out.astype(F32)[:, None],
                                 b_down.astype(F32)[:, None]], axis=1)
        small = jnp.concatenate([small, small], axis=2)
        small = jnp.concatenate([small, b_up.astype(F32).reshape(n_layers, -1, 2 * head_dim)], axis=1)
        small = jnp.pad(small, ((0, 0), (0, PAR_ROWS - small.shape[1]), (0, 0))).reshape(-1, 2 * head_dim)
        rope = jnp.asarray(rotary_lanes(seq_len, head_dim))
        call = make_kernel(n_layers, n_z, side, docs, seq_len, d_model, n_heads, ff)
        out = call(hidden.reshape(docs * seq_len, d_model), lens, small, rope, wq, w_out, w_up, w_down)[0]
        return out.reshape(docs, seq_len, d_model)

    return jax.shard_map(local_step, mesh=mesh, in_specs=in_specs, out_specs=row_spec, check_vma=False)
```

```python
import math

import jax
import jax.numpy as jnp
import numpy as np
from jax import lax
from jax.experimental import pallas as pl
from jax.experimental.pallas import tpu as pltpu
from jax.sharding import PartitionSpec as P

MESH = pl.DeviceIdType.MESH
ROPE_BASE = 10000.0
LN_EPS = 1e-5
BF = jnp.bfloat16
F32 = jnp.float32
TILE = 256
BLOCKS = 4
PAR_ROWS = 16


def rotary_lanes(seq_len, head_dim):
    rot = head_dim // 4
    half = rot // 2
    inv_freq = (1.0 / (ROPE_BASE ** (np.arange(0, rot, 2, dtype=np.float32) / rot))).astype(np.float32)
    angles = np.arange(seq_len, dtype=np.float32)[:, None] * inv_freq[None, :]
    cos_v, sin_v = np.cos(angles), np.sin(angles)
    tab = np.zeros((3, seq_len, 2 * head_dim), np.float32)
    tab[0] = 1.0
    for base in (0, head_dim):
        tab[0, :, base:base + half] = cos_v
        tab[0, :, base + half:base + rot] = cos_v
        tab[1, :, base:base + half] = -sin_v
        tab[2, :, base + half:base + rot] = sin_v
    return tab


def make_kernel(n_layers, n_z, side, docs, seq_len, d_model, n_heads, ff):
    head_dim = d_model // n_heads
    half_rot = head_dim // 8
    tokens = docs * seq_len
    lanes = 2 * head_dim
    rows_w = d_model // (2 * n_z)
    down_rows = ff // (2 * n_z)
    n_up = ff // d_model
    far = n_z // 2
    half, quarter = rows_w // 2, rows_w // 4
    per_layer = 4 + 2 * n_up
    n_st = n_layers * per_layer
    d_cols = d_model // n_up
    parts = down_rows // rows_w
    blk = tokens // BLOCKS
    n_slots = 4 * per_layer
    n_blocks = BLOCKS * (5 + 2 * n_up) + docs

    def kernel(x_hbm, lens_ref, par_ref, rope_ref, wq_hbm, wo_hbm, wu_hbm, wd_hbm,
               out_hbm, g,
               x_s, a_s, m_s, qkv_s, ctx_s, act_s, acc_s, w_s, wd_s, st_q, st_o, st_u, st_d,
               pg, tab, tab_up,
               z_send, c_send, d_send, z_recv, x_recv, y_recv, d_recv,
               p_zsend, p_dsend, p_zrecv, p_drecv,
               x_sem, st_sem, own_sem, ld_sem, ldd_sem, out_sem):
        dp = lax.axis_index("dp")
        fs = lax.axis_index("fsdp")
        z, core = lax.div(fs, 2), lax.rem(fs, 2)
        gx, gy = lax.div(dp, side), lax.rem(dp, side)
        par = lax.rem(gx + gy, 2)
        up_z = (dp, lax.rem(z + 1, n_z) * 2 + core)
        dn_z = (dp, lax.rem(z + n_z - 1, n_z) * 2 + core)
        x_dev = (dp + side * (1 - 2 * lax.rem(gx, 2)), fs)
        y_dev = (dp + 1 - 2 * lax.rem(gy, 2), fs)
        sib = (dp, z * 2 + 1 - core)
        mine = pl.multiple_of(par * half, 16)
        mine2 = pl.multiple_of(par * half + quarter, 16)
        other = pl.multiple_of((1 - par) * half, 16)
        other2 = pl.multiple_of((1 - par) * half + quarter, 16)

        def remote(src, dst, send, recv, dev):
            return pltpu.make_async_remote_copy(src_ref=src, dst_ref=dst, send_sem=send, recv_sem=recv,
                                                device_id=dev, device_id_type=MESH)

        def same(ref, send, recv, dev):
            return remote(ref, ref, send, recv, dev)

        def view(s, zz, r0, nr):
            return g.at[s, zz, core, pl.ds(r0, nr), :]

        def around(d):
            return lax.rem(z - d + n_z, n_z), lax.rem(z + d, n_z)

        def guard(s, fn):
            if isinstance(s, int):
                if 0 <= s < n_st:
                    fn()
            else:
                pl.when(s < n_st)(fn)

        def own_send(s, src=None):
            piece = view(s, z, mine, half) if src is None else src(mine, half)
            whole = view(s, z, 0, rows_w) if src is None else src(0, rows_w)
            remote(piece, view(s, z, mine, half), z_send.at[s], z_recv.at[s, 0, 0], up_z).start()
            remote(piece, view(s, z, mine, half), z_send.at[s], z_recv.at[s, 1, 0], dn_z).start()
            remote(whole, view(s, z, 0, rows_w), d_send.at[s], d_recv.at[s], sib).start()

        def z_hop(s, d):
            lo, hi = around(d)
            if d == far:
                c_x, c_y = view(s, lo, mine, quarter), view(s, lo, mine2, quarter)
                same(c_x, z_send.at[s], z_recv.at[s, 0, d - 1], up_z).wait_recv()
                same(c_x, c_send.at[s], x_recv.at[s, 0, d - 1], x_dev).start()
                same(c_y, z_send.at[s], z_recv.at[s, 1, d - 1], dn_z).wait_recv()
                same(c_y, c_send.at[s], y_recv.at[s, 0, d - 1], y_dev).start()
                return
            for j, zz, nxt in ((0, lo, up_z), (1, hi, dn_z)):
                v = view(s, zz, mine, half)
                same(v, z_send.at[s], z_recv.at[s, j, d - 1], nxt).wait_recv()
                if d == far - 1:
                    v = view(s, zz, (mine, mine2)[j], quarter)
                same(v, z_send.at[s], z_recv.at[s, j, d], nxt).start()
                c_x, c_y = view(s, zz, mine, quarter), view(s, zz, mine2, quarter)
                same(c_x, c_send.at[s], x_recv.at[s, j, d - 1], x_dev).start()
                same(c_y, c_send.at[s], y_recv.at[s, j, d - 1], y_dev).start()

        def d_hop(s, d):
            for j, zz in enumerate(around(d)[:1 if d == far else 2]):
                c_x, c_y = view(s, zz, other, quarter), view(s, zz, other2, quarter)
                same(c_x, c_send.at[s], x_recv.at[s, j, d - 1], x_dev).wait_recv()
                same(c_y, c_send.at[s], y_recv.at[s, j, d - 1], y_dev).wait_recv()
                same(view(s, zz, 0, rows_w), d_send.at[s], d_recv.at[s], sib).start()

        def slot(t, k):
            for s, d in (((t, 1),), ((t - 1, 2),), ((t - 3, 4), (t - 2, 3)), ())[k]:
                guard(s, lambda s=s, d=d: z_hop(s, d))
            for s, d in (((t - 1, 1),), ((t - 2, 2),), ((t - 4, 4), (t - 3, 3)), ())[k]:
                guard(s, lambda s=s, d=d: d_hop(s, d))
            if k == 3:
                guard(t + 2, lambda: own_send(t + 2))

        def slots_at(layer, b):
            at = lax.div(b * n_slots, n_blocks)
            prev = lax.div(b * n_slots - n_slots + n_blocks, n_blocks) - 1
            t = layer * per_layer + far + 1 + lax.div(at, 4)
            for k in range(4):
                @pl.when((at != prev) & (lax.rem(at, 4) == k))
                def _():
                    slot(t, k)

        def loads(s, slot, down):
            if not down:
                return [pltpu.make_async_copy(g.at[s], w_s.at[slot], ld_sem.at[slot])]
            return [pltpu.make_async_copy(g.at[s, :, :, :, pl.ds(q * d_cols, d_cols)],
                                          wd_s.at[slot, :, :, pl.ds(q * rows_w, rows_w), :], ldd_sem.at[slot, q])
                    for q in range(parts)]

        def fetch(s, slot, down=False):
            sibs = g.at[s, :, 1 - core]
            same(sibs, d_send.at[s], d_recv.at[s], sib).wait_recv()
            for cp in loads(s, slot, down):
                cp.start()

        x_copy = pltpu.make_async_copy(x_hbm, x_s, x_sem)
        st = [pltpu.make_async_copy(src, dst, st_sem.at[j]) for j, (src, dst) in
              enumerate(((wq_hbm, st_q), (wo_hbm, st_o), (wu_hbm, st_u), (wd_hbm, st_d)))]
        for cp in st:
            cp.start()
        x_copy.start()
        barrier = pltpu.get_barrier_semaphore()
        for dev in (up_z, dn_z, x_dev, y_dev, sib):
            pl.semaphore_signal(barrier, inc=1, device_id=dev, device_id_type=MESH)
        pl.semaphore_wait(barrier, 5)

        remote(par_ref, pg.at[z, core], p_zsend, p_zrecv.at[0, 0], up_z).start()
        remote(par_ref, pg.at[z, core], p_zsend, p_zrecv.at[1, 0], dn_z).start()
        remote(par_ref, pg.at[z, core], p_dsend, p_drecv, sib).start()
        for s in range(2):
            own_send(s, lambda r0, nr, s=s: wq_hbm.at[0, pl.ds(r0, nr), pl.ds(s * d_model, d_model)])
        pg[z, core] = par_ref[...]
        for cp in st:
            cp.wait()
        own = []
        for layer in range(n_layers):
            pieces = [(0, st_q.at[layer, :, pl.ds(j * d_model, d_model)], j) for j in range(3)]
            pieces.append((0, st_o.at[layer], 3))
            pieces += [(0, st_u.at[layer, :, pl.ds(j * d_model, d_model)], 4 + j) for j in range(n_up)]
            for j in range(n_up):
                for q in range(parts):
                    pieces.append((q, st_d.at[layer, pl.ds(q * rows_w, rows_w), pl.ds(j * d_cols, d_cols)], 4 + n_up + j))
            for q, src, j in pieces:
                dst = g.at[layer * per_layer + j, z, core]
                if j >= 4 + n_up:
                    dst = g.at[layer * per_layer + j, z, core, :, pl.ds(q * d_cols, d_cols)]
                own.append(pltpu.make_async_copy(src, dst, own_sem.at[len(own)]))
        for cp in own:
            cp.start()
        for cp in own:
            cp.wait()

        def p_hop(d):
            lo, hi = around(d)
            v_lo, v_hi = pg.at[lo, core], pg.at[hi, core]
            same(v_lo, p_zsend, p_zrecv.at[0, d - 1], up_z).wait_recv()
            if d < far:
                same(v_lo, p_zsend, p_zrecv.at[0, d], up_z).start()
                same(v_hi, p_zsend, p_zrecv.at[1, d - 1], dn_z).wait_recv()
            if d < far - 1:
                same(v_hi, p_zsend, p_zrecv.at[1, d], dn_z).start()
            same(v_lo, p_dsend, p_drecv, sib).start()
            if d < far:
                same(v_hi, p_dsend, p_drecv, sib).start()

        for t in range(far + 1):
            if t < far:
                p_hop(t + 1)
            for k in range(4):
                slot(t, k)

        p_all = pg.at[:, 1 - core]
        same(p_all, p_dsend, p_drecv, sib).wait_recv()
        low = lax.broadcasted_iota(jnp.int32, (PAR_ROWS, lanes), 1) < head_dim
        for layer in range(n_layers):
            r0 = layer * PAR_ROWS
            for zz in range(n_z):
                tab[layer, :, zz * lanes:(zz + 1) * lanes] = jnp.where(
                    low, pg[zz, 0, r0:r0 + PAR_ROWS, :], pg[zz, 1, r0:r0 + PAR_ROWS, :])
                for cc in range(2):
                    at = (zz * 2 + cc) * down_rows
                    for j in range(down_rows // lanes):
                        r = r0 + 9 + j
                        tab_up[layer, 0:1, at + j * lanes:at + (j + 1) * lanes] = pg[zz, cc, r:r + 1, :]
            for b in range(3 * n_z):
                two = []
                for p in (2 * b, 2 * b + 1):
                    dev, r = p // 3, r0 + 4 + p % 3
                    two.append(pg[dev // 2, dev % 2, r:r + 1, :])
                c0 = (b % n_z) * lanes
                tab[layer, 4 + b // n_z:5 + b // n_z, c0:c0 + lanes] = jnp.where(low[0:1], two[0], two[1])

        def norms(layer, r):
            @pl.loop(0, blk // 64)
            def _(t):
                rows = pl.ds(pl.multiple_of(r * blk + t * 64, 64), 64)
                xf = x_s[rows, :].astype(F32)
                mean = jnp.mean(xf, axis=-1, keepdims=True)
                cen = xf - mean
                var = jnp.mean(cen * cen, axis=-1, keepdims=True)
                nrm = cen * lax.rsqrt(var + LN_EPS)
                a_s[rows, :] = (nrm * tab[layer, 0:1, :] + tab[layer, 1:2, :]).astype(BF)
                m_s[rows, :] = (nrm * tab[layer, 2:3, :] + tab[layer, 3:4, :]).astype(BF)

        def dot(a, b):
            return jnp.dot(a, b, preferred_element_type=F32)

        def rows_of(r):
            return pl.ds(pl.multiple_of(r * blk, blk), blk)

        def w_tile(slot, c0, nc):
            return w_s[slot, :, :, :, c0:c0 + nc].reshape(d_model, nc)

        def qkv_block(layer, j, slot, r):
            rows = rows_of(r)
            for c0 in range(0, d_model, TILE):
                y = dot(a_s[rows, :], w_tile(slot, c0, TILE)) + tab[layer, pl.ds(4 + j, 1), c0:c0 + TILE]
                qkv_s[j, rows, c0:c0 + TILE] = y.astype(BF)

        def attend(n):
            rows = pl.ds(pl.multiple_of(n * seq_len, seq_len), seq_len)
            pos_q = lax.broadcasted_iota(jnp.int32, (seq_len, seq_len), 0)
            pos_k = lax.broadcasted_iota(jnp.int32, (seq_len, seq_len), 1)
            vis = pos_k <= jnp.minimum(pos_q, lens_ref[n] - 1)
            first = lax.broadcasted_iota(jnp.int32, (seq_len, lanes), 1) < head_dim
            zero = jnp.zeros((seq_len, lanes), BF)

            def rope(v):
                v = v.astype(F32)
                return (v * rope_ref[0] + pltpu.roll(v, lanes - half_rot, 1) * rope_ref[1]
                        + pltpu.roll(v, half_rot, 1) * rope_ref[2]).astype(BF)

            for p in range(n_heads // 2):
                cs = slice(p * lanes, (p + 1) * lanes)
                trio = []
                for b in range(3 * p, 3 * p + 3):
                    trio.append(qkv_s[b // n_z, rows, (b % n_z) * lanes:(b % n_z + 1) * lanes])
                q2 = rope(jnp.where(first, trio[0], trio[1]))
                k2 = rope(pltpu.roll(jnp.where(first, trio[2], trio[0]).astype(F32), head_dim, 1))
                v2 = jnp.where(first, trio[1], trio[2])
                kk = jnp.concatenate([jnp.where(first, k2, zero), jnp.where(first, zero, k2)], axis=0)
                vv = jnp.concatenate([jnp.where(first, v2, zero), jnp.where(first, zero, v2)], axis=0)
                sc = lax.dot_general(q2, kk, (((1,), (1,)), ((), ())), preferred_element_type=F32)
                probs = []
                for j in range(2):
                    s1 = jnp.where(vis, sc[:, j * seq_len:(j + 1) * seq_len] * (head_dim ** -0.5), -1e30)
                    e = jnp.exp(s1 - jnp.max(s1, axis=-1, keepdims=True))
                    probs.append((e * (1.0 / jnp.sum(e, axis=-1, keepdims=True))).astype(BF))
                ctx_s[rows, cs] = dot(jnp.concatenate(probs, axis=1), vv).astype(BF)

        def out_block(layer, slot, r):
            rows = rows_of(r)
            for c0 in range(0, d_model, TILE):
                cols = slice(c0, c0 + TILE)
                o = dot(ctx_s[rows, :], w_tile(slot, c0, TILE)) + tab[layer, 7:8, cols]
                acc_s[rows, cols] = x_s[rows, cols].astype(F32) + o

        def up_block(layer, j, slot, r):
            rows = rows_of(r)
            for c0 in range(0, d_model, TILE):
                cols = pl.ds(pl.multiple_of(j * d_model + c0, TILE), TILE)
                u = dot(m_s[rows, :], w_tile(slot, c0, TILE)) + tab_up[layer, 0:1, cols]
                act_s[rows, cols] = (u * 0.5 * (1.0 + lax.erf(u * (2.0 ** -0.5)))).astype(BF)

        def down_block(layer, j, slot, r):
            rows = rows_of(r)
            cols = pl.ds(pl.multiple_of(j * d_cols, d_cols), d_cols)
            w = wd_s[slot].reshape(ff, d_cols)
            y = acc_s[rows, cols] + (dot(act_s[rows, :], w) + tab[layer, 8:9, cols])
            x_s[rows, cols] = y.astype(BF)

        def out_copy(j):
            cols = pl.ds(pl.multiple_of(j * d_cols, d_cols), d_cols)
            return pltpu.make_async_copy(x_s.at[:, cols], out_hbm.at[:, cols], out_sem.at[j])

        x_copy.wait()

        @pl.loop(0, n_layers)
        def _(layer):
            s0 = layer * per_layer

            @pl.loop(0, BLOCKS)
            def _(r):
                slots_at(layer, r)

                @pl.when(r == 1)
                def _():
                    fetch(s0, 0)

                norms(layer, r)

            @pl.loop(0, 3)
            def _(j):
                buf = lax.rem(j, 2)

                @pl.loop(0, BLOCKS)
                def _(r):
                    slots_at(layer, BLOCKS * (j + 1) + r)

                    @pl.when(r == 0)
                    def _():
                        loads(s0 + j, buf, False)[0].wait()

                    @pl.when(r == 1)
                    def _():
                        fetch(s0 + j + 1, 1 - buf)

                    qkv_block(layer, j, buf, r)

            @pl.loop(0, docs)
            def _(n):
                slots_at(layer, 4 * BLOCKS + n)

                @pl.when(n == docs - 2)
                def _():
                    fetch(s0 + 4, 0)

                attend(n)

            loads(s0 + 3, 1, False)[0].wait()

            @pl.loop(0, BLOCKS)
            def _(r):
                slots_at(layer, 4 * BLOCKS + docs + r)
                out_block(layer, 1, r)

            @pl.loop(0, n_up)
            def _(j):
                buf = lax.rem(j, 2)

                @pl.loop(0, BLOCKS)
                def _(r):
                    slots_at(layer, (5 + j) * BLOCKS + docs + r)

                    @pl.when(r == 0)
                    def _():
                        loads(s0 + 4 + j, buf, False)[0].wait()

                    @pl.when((r == 1) & (j < n_up - 1))
                    def _():
                        fetch(s0 + 5 + j, 1 - buf)

                    @pl.when((r == 1) & (j == n_up - 1))
                    def _():
                        fetch(s0 + 4 + n_up, 0, True)

                    up_block(layer, j, buf, r)

            @pl.loop(0, n_up)
            def _(j):
                buf = lax.rem(j, 2)

                @pl.loop(0, BLOCKS)
                def _(r):
                    slots_at(layer, (5 + n_up + j) * BLOCKS + docs + r)

                    @pl.when(r == 0)
                    def _():
                        for cp in loads(s0 + 4 + n_up + j, buf, True):
                            cp.wait()

                    @pl.when((r == 1) & (j < n_up - 1))
                    def _():
                        fetch(s0 + 5 + n_up + j, 1 - buf, True)

                    down_block(layer, j, buf, r)

                @pl.when(layer == n_layers - 1)
                def _():
                    out_copy(j).start()

        @pl.loop(0, n_st)
        def _(s):
            sevenths = g.at[s, pl.ds(0, n_z - 1), 0, pl.ds(0, half), :]
            same(sevenths, z_send.at[s], z_recv.at[s, 0, 0], up_z).wait_send()
            same(sevenths, c_send.at[s], z_recv.at[s, 0, 0], up_z).wait_send()
            same(g.at[s, :, 0], d_send.at[s], d_recv.at[s], sib).wait_send()

        seven = pg.at[pl.ds(0, n_z - 1), 0]
        same(seven, p_zsend, p_drecv, up_z).wait_send()
        eight = pg.at[:, 0]
        same(eight, p_dsend, p_drecv, sib).wait_send()
        for j in range(n_up):
            out_copy(j).wait()

    out_shape = (
        jax.ShapeDtypeStruct((tokens, d_model), BF),
        jax.ShapeDtypeStruct((n_st, n_z, 2, rows_w, d_model), BF),
    )
    dma = pltpu.SemaphoreType.DMA
    n_own = n_layers * (4 + n_up + n_up * parts)
    act = pltpu.VMEM((tokens, d_model), BF)
    scratch = [
        act, act, act, pltpu.VMEM((3, tokens, d_model), BF), act, pltpu.VMEM((tokens, ff), BF),
        pltpu.VMEM((tokens, d_model), F32),
        pltpu.VMEM((2, n_z, 2, rows_w, d_model), BF), pltpu.VMEM((2, n_z, 2, down_rows, d_cols), BF),
        pltpu.VMEM((n_layers, rows_w, 3 * d_model), BF), pltpu.VMEM((n_layers, rows_w, d_model), BF),
        pltpu.VMEM((n_layers, rows_w, ff), BF), pltpu.VMEM((n_layers, down_rows, d_model), BF),
        pltpu.VMEM((n_z, 2, n_layers * PAR_ROWS, lanes), F32),
        pltpu.VMEM((n_layers, PAR_ROWS, d_model), F32), pltpu.VMEM((n_layers, 8, ff), F32),
        dma((n_st,)), dma((n_st,)), dma((n_st,)),
        dma((n_st, 2, far)), dma((n_st, 2, far)), dma((n_st, 2, far)), dma((n_st,)),
        dma(()), dma(()), dma((2, far)), dma(()),
        dma(()), dma((4,)), dma((n_own,)), dma((2,)), dma((2, parts)), dma((n_up,)),
    ]
    hbm = pl.BlockSpec(memory_space=pltpu.HBM)
    vmem = pl.BlockSpec(memory_space=pltpu.VMEM)
    smem = pl.BlockSpec(memory_space=pltpu.SMEM)
    return pl.pallas_call(
        kernel,
        name="layers",
        out_shape=out_shape,
        in_specs=[hbm, smem, vmem, vmem, hbm, hbm, hbm, hbm],
        out_specs=(hbm, hbm),
        scratch_shapes=scratch,
        compiler_params=pltpu.CompilerParams(collective_id=0, has_side_effects=True, vmem_limit_bytes=67043328),
    )


def solution(mesh):
    row_spec = P(('dp', 'fsdp'), None, None)
    in_specs = (row_spec, P(('dp', 'fsdp')), P(None, None, 'fsdp'), P(None, 'fsdp', None, None), P(None, 'fsdp'), P(None, 'fsdp', None), P(None, 'fsdp'), P(None, 'fsdp', None), P(None, 'fsdp'), P(None, 'fsdp', None), P(None, 'fsdp'))
    n_z = mesh.shape['fsdp'] // 2
    side = math.isqrt(mesh.shape['dp'])

    def local_step(hidden, lens, ln_par, w_qkv, b_qkv, w_out, b_out, w_up, b_up, w_down, b_down):
        docs, seq_len, d_model = hidden.shape
        n_layers, rows, n_heads, triple = w_qkv.shape
        head_dim = triple // 3
        ff = w_up.shape[2]
        wq = w_qkv.reshape(n_layers, rows, n_heads * triple)
        small = jnp.concatenate([ln_par, b_qkv.astype(F32).reshape(n_layers, 3, -1), b_out.astype(F32)[:, None],
                                 b_down.astype(F32)[:, None]], axis=1)
        small = jnp.concatenate([small, small], axis=2)
        small = jnp.concatenate([small, b_up.astype(F32).reshape(n_layers, -1, 2 * head_dim)], axis=1)
        small = jnp.pad(small, ((0, 0), (0, PAR_ROWS - small.shape[1]), (0, 0))).reshape(-1, 2 * head_dim)
        rope = jnp.asarray(rotary_lanes(seq_len, head_dim))
        call = make_kernel(n_layers, n_z, side, docs, seq_len, d_model, n_heads, ff)
        out = call(hidden.reshape(docs * seq_len, d_model), lens, small, rope, wq, w_out, w_up, w_down)[0]
        return out.reshape(docs, seq_len, d_model)

    return jax.shard_map(local_step, mesh=mesh, in_specs=in_specs, out_specs=row_spec, check_vma=False)
```

```python
import math

import jax
import jax.numpy as jnp
import numpy as np
from jax import lax
from jax.experimental import pallas as pl
from jax.experimental.pallas import tpu as pltpu
from jax.sharding import PartitionSpec as P

MESH = pl.DeviceIdType.MESH
ROPE_BASE = 10000.0
LN_EPS = 1e-5
BF = jnp.bfloat16
F32 = jnp.float32
TILE = 256
BLOCKS = 4
PAR_ROWS = 16


def rotary_lanes(seq_len, head_dim):
    rot = head_dim // 4
    half = rot // 2
    inv_freq = (1.0 / (ROPE_BASE ** (np.arange(0, rot, 2, dtype=np.float32) / rot))).astype(np.float32)
    angles = np.arange(seq_len, dtype=np.float32)[:, None] * inv_freq[None, :]
    cos_v, sin_v = np.cos(angles), np.sin(angles)
    tab = np.zeros((3, seq_len, 2 * head_dim), np.float32)
    tab[0] = 1.0
    for base in (0, head_dim):
        tab[0, :, base:base + half] = cos_v
        tab[0, :, base + half:base + rot] = cos_v
        tab[1, :, base:base + half] = -sin_v
        tab[2, :, base + half:base + rot] = sin_v
    return tab


def make_kernel(n_layers, n_z, side, docs, seq_len, d_model, n_heads, ff):
    head_dim = d_model // n_heads
    half_rot = head_dim // 8
    tokens = docs * seq_len
    lanes = 2 * head_dim
    rows_w = d_model // (2 * n_z)
    down_rows = ff // (2 * n_z)
    n_up = ff // d_model
    far = n_z // 2
    half, quarter = rows_w // 2, rows_w // 4
    per_layer = 4 + 2 * n_up
    n_st = n_layers * per_layer
    d_cols = d_model // n_up
    parts = down_rows // rows_w
    blk = tokens // BLOCKS
    n_slots = 4 * per_layer
    n_blocks = BLOCKS * (5 + 2 * n_up) + docs

    def kernel(x_hbm, lens_ref, ln_ref, bq_ref, bo_ref, bu_ref, bd_ref, rope_ref, wq_hbm, wo_hbm, wu_hbm, wd_hbm,
               out_hbm, g,
               par_ref, x_s, a_s, m_s, q_r, k_r, v_r, qkv_s, ctx_s, act_s, acc_s, w_s, wd_s, st_q, st_o, st_u, st_d,
               pg, tab, tab_up,
               z_send, c_send, d_send, z_recv, x_recv, y_recv, d_recv,
               p_zsend, p_dsend, p_zrecv, p_drecv,
               x_sem, st_sem, own_sem, ld_sem, ldd_sem, out_sem):
        dp = lax.axis_index("dp")
        fs = lax.axis_index("fsdp")
        z, core = lax.div(fs, 2), lax.rem(fs, 2)
        gx, gy = lax.div(dp, side), lax.rem(dp, side)
        par = lax.rem(gx + gy, 2)
        up_z = (dp, lax.rem(z + 1, n_z) * 2 + core)
        dn_z = (dp, lax.rem(z + n_z - 1, n_z) * 2 + core)
        x_dev = (dp + side * (1 - 2 * lax.rem(gx, 2)), fs)
        y_dev = (dp + 1 - 2 * lax.rem(gy, 2), fs)
        sib = (dp, z * 2 + 1 - core)
        mine = pl.multiple_of(par * half, 16)
        mine2 = pl.multiple_of(par * half + quarter, 16)
        other = pl.multiple_of((1 - par) * half, 16)
        other2 = pl.multiple_of((1 - par) * half + quarter, 16)

        def remote(src, dst, send, recv, dev):
            return pltpu.make_async_remote_copy(src_ref=src, dst_ref=dst, send_sem=send, recv_sem=recv,
                                                device_id=dev, device_id_type=MESH)

        def same(ref, send, recv, dev):
            return remote(ref, ref, send, recv, dev)

        def view(s, zz, r0, nr):
            return g.at[s, zz, core, pl.ds(r0, nr), :]

        def around(d):
            return lax.rem(z - d + n_z, n_z), lax.rem(z + d, n_z)

        def guard(s, fn):
            if isinstance(s, int):
                if 0 <= s < n_st:
                    fn()
            else:
                pl.when(s < n_st)(fn)

        def own_send(s, src=None):
            piece = view(s, z, mine, half) if src is None else src(mine, half)
            whole = view(s, z, 0, rows_w) if src is None else src(0, rows_w)
            remote(piece, view(s, z, mine, half), z_send.at[s], z_recv.at[s, 0, 0], up_z).start()
            remote(piece, view(s, z, mine, half), z_send.at[s], z_recv.at[s, 1, 0], dn_z).start()
            remote(whole, view(s, z, 0, rows_w), d_send.at[s], d_recv.at[s], sib).start()

        def z_hop(s, d):
            lo, hi = around(d)
            if d == far:
                c_x, c_y = view(s, lo, mine, quarter), view(s, lo, mine2, quarter)
                same(c_x, z_send.at[s], z_recv.at[s, 0, d - 1], up_z).wait_recv()
                same(c_x, c_send.at[s], x_recv.at[s, 0, d - 1], x_dev).start()
                same(c_y, z_send.at[s], z_recv.at[s, 1, d - 1], dn_z).wait_recv()
                same(c_y, c_send.at[s], y_recv.at[s, 0, d - 1], y_dev).start()
                return
            for j, zz, nxt in ((0, lo, up_z), (1, hi, dn_z)):
                v = view(s, zz, mine, half)
                same(v, z_send.at[s], z_recv.at[s, j, d - 1], nxt).wait_recv()
                if d == far - 1:
                    v = view(s, zz, (mine, mine2)[j], quarter)
                same(v, z_send.at[s], z_recv.at[s, j, d], nxt).start()
                c_x, c_y = view(s, zz, mine, quarter), view(s, zz, mine2, quarter)
                same(c_x, c_send.at[s], x_recv.at[s, j, d - 1], x_dev).start()
                same(c_y, c_send.at[s], y_recv.at[s, j, d - 1], y_dev).start()

        def d_hop(s, d):
            for j, zz in enumerate(around(d)[:1 if d == far else 2]):
                c_x, c_y = view(s, zz, other, quarter), view(s, zz, other2, quarter)
                same(c_x, c_send.at[s], x_recv.at[s, j, d - 1], x_dev).wait_recv()
                same(c_y, c_send.at[s], y_recv.at[s, j, d - 1], y_dev).wait_recv()
                same(view(s, zz, 0, rows_w), d_send.at[s], d_recv.at[s], sib).start()

        def slot(t, k):
            for s, d in (((t, 1),), ((t - 1, 2),), ((t - 3, 4), (t - 2, 3)), ())[k]:
                guard(s, lambda s=s, d=d: z_hop(s, d))
            for s, d in (((t - 1, 1),), ((t - 2, 2),), ((t - 4, 4), (t - 3, 3)), ())[k]:
                guard(s, lambda s=s, d=d: d_hop(s, d))
            if k == 3:
                guard(t + 2, lambda: own_send(t + 2))

        def slots_at(layer, b):
            at = lax.div(b * n_slots, n_blocks)
            prev = lax.div(b * n_slots - n_slots + n_blocks, n_blocks) - 1
            t = layer * per_layer + far + 1 + lax.div(at, 4)
            for k in range(4):
                @pl.when((at != prev) & (lax.rem(at, 4) == k))
                def _():
                    slot(t, k)

        def loads(s, slot, down):
            if not down:
                return [pltpu.make_async_copy(g.at[s], w_s.at[slot], ld_sem.at[slot])]
            return [pltpu.make_async_copy(g.at[s, :, :, :, pl.ds(q * d_cols, d_cols)],
                                          wd_s.at[slot, :, :, pl.ds(q * rows_w, rows_w), :], ldd_sem.at[slot, q])
                    for q in range(parts)]

        def fetch(s, slot, down=False):
            sibs = g.at[s, :, 1 - core]
            same(sibs, d_send.at[s], d_recv.at[s], sib).wait_recv()
            for cp in loads(s, slot, down):
                cp.start()

        x_copy = pltpu.make_async_copy(x_hbm, x_s, x_sem)
        st = [pltpu.make_async_copy(src, dst, st_sem.at[j]) for j, (src, dst) in
              enumerate(((wq_hbm, st_q), (wo_hbm, st_o), (wu_hbm, st_u), (wd_hbm, st_d)))]
        for cp in st:
            cp.start()
        x_copy.start()

        def twice(v):
            return jnp.concatenate([v, v], axis=1)

        for layer in range(n_layers):
            r0 = layer * PAR_ROWS
            row = slice(layer, layer + 1)
            par_ref[r0:r0 + 4, :] = twice(ln_ref[layer])
            b_q = bq_ref[row, :].astype(F32)
            for j in range(3):
                par_ref[r0 + 4 + j:r0 + 5 + j, :] = twice(b_q[:, j * head_dim:(j + 1) * head_dim])
            par_ref[r0 + 7:r0 + 8, :] = twice(bo_ref[row, :].astype(F32))
            par_ref[r0 + 8:r0 + 9, :] = twice(bd_ref[row, :].astype(F32))
            for j in range(down_rows // lanes):
                par_ref[r0 + 9 + j:r0 + 10 + j, :] = bu_ref[row, j * lanes:(j + 1) * lanes].astype(F32)
            r1 = 9 + down_rows // lanes
            par_ref[r0 + r1:r0 + PAR_ROWS, :] = jnp.zeros((PAR_ROWS - r1, lanes), F32)
        barrier = pltpu.get_barrier_semaphore()
        for dev in (up_z, dn_z, x_dev, y_dev, sib):
            pl.semaphore_signal(barrier, inc=1, device_id=dev, device_id_type=MESH)
        pl.semaphore_wait(barrier, 5)

        remote(par_ref, pg.at[z, core], p_zsend, p_zrecv.at[0, 0], up_z).start()
        remote(par_ref, pg.at[z, core], p_zsend, p_zrecv.at[1, 0], dn_z).start()
        remote(par_ref, pg.at[z, core], p_dsend, p_drecv, sib).start()
        for s in range(2):
            own_send(s, lambda r0, nr, s=s: wq_hbm.at[0, pl.ds(r0, nr), pl.ds(s * d_model, d_model)])
        pg[z, core] = par_ref[...]
        for cp in st:
            cp.wait()
        own = []
        for layer in range(n_layers):
            pieces = [(0, st_q.at[layer, :, pl.ds(j * d_model, d_model)], j) for j in range(3)]
            pieces.append((0, st_o.at[layer], 3))
            pieces += [(0, st_u.at[layer, :, pl.ds(j * d_model, d_model)], 4 + j) for j in range(n_up)]
            for j in range(n_up):
                for q in range(parts):
                    pieces.append((q, st_d.at[layer, pl.ds(q * rows_w, rows_w), pl.ds(j * d_cols, d_cols)], 4 + n_up + j))
            for q, src, j in pieces:
                dst = g.at[layer * per_layer + j, z, core]
                if j >= 4 + n_up:
                    dst = g.at[layer * per_layer + j, z, core, :, pl.ds(q * d_cols, d_cols)]
                own.append(pltpu.make_async_copy(src, dst, own_sem.at[len(own)]))
        for cp in own:
            cp.start()
        for cp in own:
            cp.wait()

        def p_hop(d):
            lo, hi = around(d)
            v_lo, v_hi = pg.at[lo, core], pg.at[hi, core]
            same(v_lo, p_zsend, p_zrecv.at[0, d - 1], up_z).wait_recv()
            if d < far:
                same(v_lo, p_zsend, p_zrecv.at[0, d], up_z).start()
                same(v_hi, p_zsend, p_zrecv.at[1, d - 1], dn_z).wait_recv()
            if d < far - 1:
                same(v_hi, p_zsend, p_zrecv.at[1, d], dn_z).start()
            same(v_lo, p_dsend, p_drecv, sib).start()
            if d < far:
                same(v_hi, p_dsend, p_drecv, sib).start()

        for t in range(far + 1):
            if t < far:
                p_hop(t + 1)
            for k in range(4):
                slot(t, k)

        p_all = pg.at[:, 1 - core]
        same(p_all, p_dsend, p_drecv, sib).wait_recv()
        low = lax.broadcasted_iota(jnp.int32, (PAR_ROWS, lanes), 1) < head_dim
        for layer in range(n_layers):
            r0 = layer * PAR_ROWS
            for zz in range(n_z):
                tab[layer, :, zz * lanes:(zz + 1) * lanes] = jnp.where(
                    low, pg[zz, 0, r0:r0 + PAR_ROWS, :], pg[zz, 1, r0:r0 + PAR_ROWS, :])
                for cc in range(2):
                    at = (zz * 2 + cc) * down_rows
                    for j in range(down_rows // lanes):
                        r = r0 + 9 + j
                        tab_up[layer, 0:1, at + j * lanes:at + (j + 1) * lanes] = pg[zz, cc, r:r + 1, :]
            for b in range(3 * n_z):
                two = []
                for p in (2 * b, 2 * b + 1):
                    dev, r = p // 3, r0 + 4 + p % 3
                    two.append(pg[dev // 2, dev % 2, r:r + 1, :])
                c0 = (b % n_z) * lanes
                tab[layer, 4 + b // n_z:5 + b // n_z, c0:c0 + lanes] = jnp.where(low[0:1], two[0], two[1])

        def norms(layer, r):
            @pl.loop(0, blk // 64)
            def _(t):
                rows = pl.ds(pl.multiple_of(r * blk + t * 64, 64), 64)
                xf = x_s[rows, :].astype(F32)
                mean = jnp.mean(xf, axis=-1, keepdims=True)
                cen = xf - mean
                var = jnp.mean(cen * cen, axis=-1, keepdims=True)
                nrm = cen * lax.rsqrt(var + LN_EPS)
                a_s[rows, :] = (nrm * tab[layer, 0:1, :] + tab[layer, 1:2, :]).astype(BF)
                m_s[rows, :] = (nrm * tab[layer, 2:3, :] + tab[layer, 3:4, :]).astype(BF)

        def dot(a, b):
            return jnp.dot(a, b, preferred_element_type=F32)

        def rows_of(r):
            return pl.ds(pl.multiple_of(r * blk, blk), blk)

        def w_tile(slot, c0, nc):
            return w_s[slot, :, :, :, c0:c0 + nc].reshape(d_model, nc)

        def qkv_block(layer, j, slot, r):
            rows = rows_of(r)
            for c0 in range(0, d_model, TILE):
                y = dot(a_s[rows, :], w_tile(slot, c0, TILE)) + tab[layer, pl.ds(4 + j, 1), c0:c0 + TILE]
                qkv_s[j, rows, c0:c0 + TILE] = y.astype(BF)

        def attend(n):
            rows = pl.ds(pl.multiple_of(n * seq_len, seq_len), seq_len)
            pos_q = lax.broadcasted_iota(jnp.int32, (seq_len, seq_len), 0)
            pos_k = lax.broadcasted_iota(jnp.int32, (seq_len, seq_len), 1)
            vis = pos_k <= jnp.minimum(pos_q, lens_ref[n] - 1)
            first = lax.broadcasted_iota(jnp.int32, (seq_len, lanes), 1) < head_dim
            zero = jnp.zeros((seq_len, lanes), BF)

            def rope(v):
                return (v * rope_ref[0] + pltpu.roll(v, lanes - half_rot, 1) * rope_ref[1]
                        + pltpu.roll(v, half_rot, 1) * rope_ref[2]).astype(BF)

            for p in range(n_heads // 2):
                cs = slice(p * lanes, (p + 1) * lanes)
                trio = []
                for b in range(3 * p, 3 * p + 3):
                    trio.append(qkv_s[b // n_z, rows, (b % n_z) * lanes:(b % n_z + 1) * lanes])
                q_r[:, cs] = rope(jnp.where(first, trio[0], trio[1]).astype(F32))
                k_r[:, cs] = rope(pltpu.roll(jnp.where(first, trio[2], trio[0]).astype(F32), head_dim, 1))
                v_r[:, cs] = jnp.where(first, trio[1], trio[2])

            for p in range(n_heads // 2):
                cs = slice(p * lanes, (p + 1) * lanes)
                k2, v2 = k_r[:, cs], v_r[:, cs]
                kk = jnp.concatenate([jnp.where(first, k2, zero), jnp.where(first, zero, k2)], axis=0)
                vv = jnp.concatenate([jnp.where(first, v2, zero), jnp.where(first, zero, v2)], axis=0)
                sc = lax.dot_general(q_r[:, cs], kk, (((1,), (1,)), ((), ())), preferred_element_type=F32)
                probs = []
                for j in range(2):
                    s1 = jnp.where(vis, sc[:, j * seq_len:(j + 1) * seq_len] * (head_dim ** -0.5 * math.log2(math.e)), -1e30)
                    e = jnp.exp2(s1 - jnp.max(s1, axis=-1, keepdims=True))
                    probs.append((e * (1.0 / jnp.sum(e, axis=-1, keepdims=True))).astype(BF))
                ctx_s[rows, cs] = dot(jnp.concatenate(probs, axis=1), vv).astype(BF)

        def out_block(layer, slot, r):
            rows = rows_of(r)
            for c0 in range(0, d_model, TILE):
                cols = slice(c0, c0 + TILE)
                o = dot(ctx_s[rows, :], w_tile(slot, c0, TILE)) + tab[layer, 7:8, cols]
                acc_s[rows, cols] = x_s[rows, cols].astype(F32) + o

        def up_block(layer, j, slot, r):
            rows = rows_of(r)
            for c0 in range(0, d_model, TILE):
                cols = pl.ds(pl.multiple_of(j * d_model + c0, TILE), TILE)
                u = dot(m_s[rows, :], w_tile(slot, c0, TILE)) + tab_up[layer, 0:1, cols]
                act_s[rows, cols] = (u * 0.5 * (1.0 + lax.erf(u * (2.0 ** -0.5)))).astype(BF)

        def down_block(layer, j, slot, r):
            rows = rows_of(r)
            cols = pl.ds(pl.multiple_of(j * d_cols, d_cols), d_cols)
            w = wd_s[slot].reshape(ff, d_cols)
            y = acc_s[rows, cols] + (dot(act_s[rows, :], w) + tab[layer, 8:9, cols])
            x_s[rows, cols] = y.astype(BF)

        def out_copy(j):
            cols = pl.ds(pl.multiple_of(j * d_cols, d_cols), d_cols)
            return pltpu.make_async_copy(x_s.at[:, cols], out_hbm.at[:, cols], out_sem.at[j])

        x_copy.wait()

        @pl.loop(0, n_layers)
        def _(layer):
            s0 = layer * per_layer

            @pl.loop(0, BLOCKS)
            def _(r):
                slots_at(layer, r)

                @pl.when(r == 1)
                def _():
                    fetch(s0, 0)

                norms(layer, r)

            @pl.loop(0, 3)
            def _(j):
                buf = lax.rem(j, 2)

                @pl.loop(0, BLOCKS)
                def _(r):
                    slots_at(layer, BLOCKS * (j + 1) + r)

                    @pl.when(r == 0)
                    def _():
                        loads(s0 + j, buf, False)[0].wait()

                    @pl.when(r == 1)
                    def _():
                        fetch(s0 + j + 1, 1 - buf)

                    qkv_block(layer, j, buf, r)

            @pl.loop(0, docs)
            def _(n):
                slots_at(layer, 4 * BLOCKS + n)

                @pl.when(n == docs - 2)
                def _():
                    fetch(s0 + 4, 0)

                attend(n)

            loads(s0 + 3, 1, False)[0].wait()

            @pl.loop(0, BLOCKS)
            def _(r):
                slots_at(layer, 4 * BLOCKS + docs + r)
                out_block(layer, 1, r)

            @pl.loop(0, n_up)
            def _(j):
                buf = lax.rem(j, 2)

                @pl.loop(0, BLOCKS)
                def _(r):
                    slots_at(layer, (5 + j) * BLOCKS + docs + r)

                    @pl.when(r == 0)
                    def _():
                        loads(s0 + 4 + j, buf, False)[0].wait()

                    @pl.when((r == 1) & (j < n_up - 1))
                    def _():
                        fetch(s0 + 5 + j, 1 - buf)

                    @pl.when((r == 1) & (j == n_up - 1))
                    def _():
                        fetch(s0 + 4 + n_up, 0, True)

                    up_block(layer, j, buf, r)

            @pl.loop(0, n_up)
            def _(j):
                buf = lax.rem(j, 2)

                @pl.loop(0, BLOCKS)
                def _(r):
                    slots_at(layer, (5 + n_up + j) * BLOCKS + docs + r)

                    @pl.when(r == 0)
                    def _():
                        for cp in loads(s0 + 4 + n_up + j, buf, True):
                            cp.wait()

                    @pl.when((r == 1) & (j < n_up - 1))
                    def _():
                        fetch(s0 + 5 + n_up + j, 1 - buf, True)

                    down_block(layer, j, buf, r)

                @pl.when(layer == n_layers - 1)
                def _():
                    out_copy(j).start()

        @pl.loop(0, n_st)
        def _(s):
            sevenths = g.at[s, pl.ds(0, n_z - 1), 0, pl.ds(0, half), :]
            same(sevenths, z_send.at[s], z_recv.at[s, 0, 0], up_z).wait_send()
            same(sevenths, c_send.at[s], z_recv.at[s, 0, 0], up_z).wait_send()
            same(g.at[s, :, 0], d_send.at[s], d_recv.at[s], sib).wait_send()

        seven = pg.at[pl.ds(0, n_z - 1), 0]
        same(seven, p_zsend, p_drecv, up_z).wait_send()
        eight = pg.at[:, 0]
        same(eight, p_dsend, p_drecv, sib).wait_send()
        for j in range(n_up):
            out_copy(j).wait()

    out_shape = (
        jax.ShapeDtypeStruct((tokens, d_model), BF),
        jax.ShapeDtypeStruct((n_st, n_z, 2, rows_w, d_model), BF),
    )
    dma = pltpu.SemaphoreType.DMA
    n_own = n_layers * (4 + n_up + n_up * parts)
    act = pltpu.VMEM((tokens, d_model), BF)
    doc_v = pltpu.VMEM((seq_len, d_model), BF)
    scratch = [
        pltpu.VMEM((n_layers * PAR_ROWS, lanes), F32), act, act, act, doc_v, doc_v, doc_v, pltpu.VMEM((3, tokens, d_model), BF), act, pltpu.VMEM((tokens, ff), BF),
        pltpu.VMEM((tokens, d_model), F32),
        pltpu.VMEM((2, n_z, 2, rows_w, d_model), BF), pltpu.VMEM((2, n_z, 2, down_rows, d_cols), BF),
        pltpu.VMEM((n_layers, rows_w, 3 * d_model), BF), pltpu.VMEM((n_layers, rows_w, d_model), BF),
        pltpu.VMEM((n_layers, rows_w, ff), BF), pltpu.VMEM((n_layers, down_rows, d_model), BF),
        pltpu.VMEM((n_z, 2, n_layers * PAR_ROWS, lanes), F32),
        pltpu.VMEM((n_layers, PAR_ROWS, d_model), F32), pltpu.VMEM((n_layers, 8, ff), F32),
        dma((n_st,)), dma((n_st,)), dma((n_st,)),
        dma((n_st, 2, far)), dma((n_st, 2, far)), dma((n_st, 2, far)), dma((n_st,)),
        dma(()), dma(()), dma((2, far)), dma(()),
        dma(()), dma((4,)), dma((n_own,)), dma((2,)), dma((2, parts)), dma((n_up,)),
    ]
    hbm = pl.BlockSpec(memory_space=pltpu.HBM)
    vmem = pl.BlockSpec(memory_space=pltpu.VMEM)
    smem = pl.BlockSpec(memory_space=pltpu.SMEM)
    return pl.pallas_call(
        kernel,
        name="layers",
        out_shape=out_shape,
        in_specs=[hbm, smem] + [vmem] * 6 + [hbm] * 4,
        out_specs=(hbm, hbm),
        scratch_shapes=scratch,
        compiler_params=pltpu.CompilerParams(collective_id=0, has_side_effects=True, vmem_limit_bytes=67043328),
    )


def solution(mesh):
    row_spec = P(('dp', 'fsdp'), None, None)
    in_specs = (row_spec, P(('dp', 'fsdp')), P(None, None, 'fsdp'), P(None, 'fsdp', None, None), P(None, 'fsdp'), P(None, 'fsdp', None), P(None, 'fsdp'), P(None, 'fsdp', None), P(None, 'fsdp'), P(None, 'fsdp', None), P(None, 'fsdp'))
    n_z = mesh.shape['fsdp'] // 2
    side = math.isqrt(mesh.shape['dp'])

    def local_step(hidden, lens, ln_par, w_qkv, b_qkv, w_out, b_out, w_up, b_up, w_down, b_down):
        docs, seq_len, d_model = hidden.shape
        n_layers, rows, n_heads, triple = w_qkv.shape
        head_dim = triple // 3
        ff = w_up.shape[2]
        wq = w_qkv.reshape(n_layers, rows, n_heads * triple)
        call = make_kernel(n_layers, n_z, side, docs, seq_len, d_model, n_heads, ff)
        out = call(hidden.reshape(docs * seq_len, d_model), lens, ln_par, b_qkv, b_out, b_up, b_down, jnp.asarray(rotary_lanes(seq_len, head_dim)),
                   wq, w_out, w_up, w_down)[0]
        return out.reshape(docs, seq_len, d_model)

    return jax.shard_map(local_step, mesh=mesh, in_specs=in_specs, out_specs=row_spec, check_vma=False)
```

```python
import math

import jax
import jax.numpy as jnp
import numpy as np
from jax import lax
from jax.experimental import pallas as pl
from jax.experimental.pallas import tpu as pltpu
from jax.sharding import PartitionSpec as P

MESH = pl.DeviceIdType.MESH
ROPE_BASE = 10000.0
LN_EPS = 1e-5
BF = jnp.bfloat16
F32 = jnp.float32
TILE = 256
BLOCKS = 4
PAR_ROWS = 16


def rotary_lanes(seq_len, head_dim):
    rot = head_dim // 4
    half = rot // 2
    inv_freq = (1.0 / (ROPE_BASE ** (np.arange(0, rot, 2, dtype=np.float32) / rot))).astype(np.float32)
    angles = np.arange(seq_len, dtype=np.float32)[:, None] * inv_freq[None, :]
    cos_v, sin_v = np.cos(angles), np.sin(angles)
    tab = np.zeros((2, seq_len, 2 * head_dim), np.float32)
    tab[0] = 1.0
    for base in (0, head_dim):
        tab[0, :, base:base + half] = cos_v
        tab[0, :, base + half:base + rot] = cos_v
        tab[1, :, base:base + half] = -sin_v
        tab[1, :, base + half:base + rot] = sin_v
    return tab


def make_kernel(n_layers, n_z, side, docs, seq_len, d_model, n_heads, ff):
    head_dim = d_model // n_heads
    half_rot = head_dim // 8
    tokens = docs * seq_len
    lanes = 2 * head_dim
    rows_w = d_model // (2 * n_z)
    down_rows = ff // (2 * n_z)
    n_up = ff // d_model
    far = n_z // 2
    half, quarter = rows_w // 2, rows_w // 4
    per_layer = 4 + 2 * n_up
    n_st = n_layers * per_layer
    d_cols = d_model // n_up
    parts = down_rows // rows_w
    blk = tokens // BLOCKS
    n_slots = 4 * per_layer
    n_blocks = BLOCKS * (5 + 2 * n_up) + docs

    def kernel(x_hbm, lens_ref, ln_ref, bq_ref, bo_ref, bu_ref, bd_ref, rope_ref, wq_hbm, wo_hbm, wu_hbm, wd_hbm,
               out_hbm, g,
               par_ref, x_s, a_s, m_s, q_r, k_r, v_r, qkv_s, ctx_s, act_s, acc_s, w_s, wd_s, st_q, st_o, st_u, st_d,
               pg, tab, tab_up,
               z_send, c_send, d_send, z_recv, x_recv, y_recv, d_recv,
               p_zsend, p_dsend, p_zrecv, p_drecv,
               x_sem, st_sem, own_sem, ld_sem, ldd_sem, out_sem):
        dp = lax.axis_index("dp")
        fs = lax.axis_index("fsdp")
        z, core = lax.div(fs, 2), lax.rem(fs, 2)
        gx, gy = lax.div(dp, side), lax.rem(dp, side)
        par = lax.rem(gx + gy, 2)
        up_z = (dp, lax.rem(z + 1, n_z) * 2 + core)
        dn_z = (dp, lax.rem(z + n_z - 1, n_z) * 2 + core)
        x_dev = (dp + side * (1 - 2 * lax.rem(gx, 2)), fs)
        y_dev = (dp + 1 - 2 * lax.rem(gy, 2), fs)
        sib = (dp, z * 2 + 1 - core)
        mine = pl.multiple_of(par * half, 16)
        mine2 = pl.multiple_of(par * half + quarter, 16)
        other = pl.multiple_of((1 - par) * half, 16)
        other2 = pl.multiple_of((1 - par) * half + quarter, 16)

        def remote(src, dst, send, recv, dev):
            return pltpu.make_async_remote_copy(src_ref=src, dst_ref=dst, send_sem=send, recv_sem=recv,
                                                device_id=dev, device_id_type=MESH)

        def same(ref, send, recv, dev):
            return remote(ref, ref, send, recv, dev)

        def view(s, zz, r0, nr):
            return g.at[s, zz, core, pl.ds(r0, nr), :]

        def around(d):
            return lax.rem(z - d + n_z, n_z), lax.rem(z + d, n_z)

        def guard(s, fn):
            if isinstance(s, int):
                if 0 <= s < n_st:
                    fn()
            else:
                pl.when(s < n_st)(fn)

        def own_send(s, src=None):
            piece = view(s, z, mine, half) if src is None else src(mine, half)
            whole = view(s, z, 0, rows_w) if src is None else src(0, rows_w)
            remote(piece, view(s, z, mine, half), z_send.at[s], z_recv.at[s, 0, 0], up_z).start()
            remote(piece, view(s, z, mine, half), z_send.at[s], z_recv.at[s, 1, 0], dn_z).start()
            remote(whole, view(s, z, 0, rows_w), d_send.at[s], d_recv.at[s], sib).start()

        def z_hop(s, d):
            lo, hi = around(d)
            if d == far:
                c_x, c_y = view(s, lo, mine, quarter), view(s, lo, mine2, quarter)
                same(c_x, z_send.at[s], z_recv.at[s, 0, d - 1], up_z).wait_recv()
                same(c_x, c_send.at[s], x_recv.at[s, 0, d - 1], x_dev).start()
                same(c_y, z_send.at[s], z_recv.at[s, 1, d - 1], dn_z).wait_recv()
                same(c_y, c_send.at[s], y_recv.at[s, 0, d - 1], y_dev).start()
                return
            for j, zz, nxt in ((0, lo, up_z), (1, hi, dn_z)):
                v = view(s, zz, mine, half)
                same(v, z_send.at[s], z_recv.at[s, j, d - 1], nxt).wait_recv()
                if d == far - 1:
                    v = view(s, zz, (mine, mine2)[j], quarter)
                same(v, z_send.at[s], z_recv.at[s, j, d], nxt).start()
                c_x, c_y = view(s, zz, mine, quarter), view(s, zz, mine2, quarter)
                same(c_x, c_send.at[s], x_recv.at[s, j, d - 1], x_dev).start()
                same(c_y, c_send.at[s], y_recv.at[s, j, d - 1], y_dev).start()

        def d_hop(s, d):
            for j, zz in enumerate(around(d)[:1 if d == far else 2]):
                c_x, c_y = view(s, zz, other, quarter), view(s, zz, other2, quarter)
                same(c_x, c_send.at[s], x_recv.at[s, j, d - 1], x_dev).wait_recv()
                same(c_y, c_send.at[s], y_recv.at[s, j, d - 1], y_dev).wait_recv()
                same(view(s, zz, 0, rows_w), d_send.at[s], d_recv.at[s], sib).start()

        def slot(t, k):
            for s, d in (((t, 1),), ((t - 1, 2),), ((t - 3, 4), (t - 2, 3)), ())[k]:
                guard(s, lambda s=s, d=d: z_hop(s, d))
            for s, d in (((t - 1, 1),), ((t - 2, 2),), ((t - 4, 4), (t - 3, 3)), ())[k]:
                guard(s, lambda s=s, d=d: d_hop(s, d))
            if k == 3:
                guard(t + 2, lambda: own_send(t + 2))

        def slots_at(layer, b):
            at = lax.div(b * n_slots, n_blocks)
            prev = lax.div(b * n_slots - n_slots + n_blocks, n_blocks) - 1
            t = layer * per_layer + far + 1 + lax.div(at, 4)
            for k in range(4):
                @pl.when((at != prev) & (lax.rem(at, 4) == k))
                def _():
                    slot(t, k)

        def loads(s, slot, down):
            if not down:
                return [pltpu.make_async_copy(g.at[s], w_s.at[slot], ld_sem.at[slot])]
            return [pltpu.make_async_copy(g.at[s, :, :, :, pl.ds(q * d_cols, d_cols)],
                                          wd_s.at[slot, :, :, pl.ds(q * rows_w, rows_w), :], ldd_sem.at[slot, q])
                    for q in range(parts)]

        def fetch(s, slot, down=False):
            sibs = g.at[s, :, 1 - core]
            same(sibs, d_send.at[s], d_recv.at[s], sib).wait_recv()
            for cp in loads(s, slot, down):
                cp.start()

        x_copy = pltpu.make_async_copy(x_hbm, x_s, x_sem)
        st = [pltpu.make_async_copy(src, dst, st_sem.at[j]) for j, (src, dst) in
              enumerate(((wq_hbm, st_q), (wo_hbm, st_o), (wu_hbm, st_u), (wd_hbm, st_d)))]
        for cp in st:
            cp.start()
        x_copy.start()

        def twice(v):
            return jnp.concatenate([v, v], axis=1)

        for layer in range(n_layers):
            r0 = layer * PAR_ROWS
            row = slice(layer, layer + 1)
            par_ref[r0:r0 + 4, :] = twice(ln_ref[layer])
            b_q = bq_ref[row, :].astype(F32)
            for j in range(3):
                par_ref[r0 + 4 + j:r0 + 5 + j, :] = twice(b_q[:, j * head_dim:(j + 1) * head_dim])
            par_ref[r0 + 7:r0 + 8, :] = twice(bo_ref[row, :].astype(F32))
            par_ref[r0 + 8:r0 + 9, :] = twice(bd_ref[row, :].astype(F32))
            for j in range(down_rows // lanes):
                par_ref[r0 + 9 + j:r0 + 10 + j, :] = bu_ref[row, j * lanes:(j + 1) * lanes].astype(F32)
            r1 = 9 + down_rows // lanes
            par_ref[r0 + r1:r0 + PAR_ROWS, :] = jnp.zeros((PAR_ROWS - r1, lanes), F32)
        barrier = pltpu.get_barrier_semaphore()
        for dev in (up_z, dn_z, x_dev, y_dev, sib):
            pl.semaphore_signal(barrier, inc=1, device_id=dev, device_id_type=MESH)
        pl.semaphore_wait(barrier, 5)

        remote(par_ref, pg.at[z, core], p_zsend, p_zrecv.at[0, 0], up_z).start()
        remote(par_ref, pg.at[z, core], p_zsend, p_zrecv.at[1, 0], dn_z).start()
        remote(par_ref, pg.at[z, core], p_dsend, p_drecv, sib).start()
        for s in range(2):
            own_send(s, lambda r0, nr, s=s: wq_hbm.at[0, pl.ds(r0, nr), pl.ds(s * d_model, d_model)])
        pg[z, core] = par_ref[...]
        for cp in st:
            cp.wait()
        own = []
        for layer in range(n_layers):
            pieces = [(0, st_q.at[layer, :, pl.ds(j * d_model, d_model)], j) for j in range(3)]
            pieces.append((0, st_o.at[layer], 3))
            pieces += [(0, st_u.at[layer, :, pl.ds(j * d_model, d_model)], 4 + j) for j in range(n_up)]
            for j in range(n_up):
                for q in range(parts):
                    pieces.append((q, st_d.at[layer, pl.ds(q * rows_w, rows_w), pl.ds(j * d_cols, d_cols)], 4 + n_up + j))
            for q, src, j in pieces:
                dst = g.at[layer * per_layer + j, z, core]
                if j >= 4 + n_up:
                    dst = g.at[layer * per_layer + j, z, core, :, pl.ds(q * d_cols, d_cols)]
                own.append(pltpu.make_async_copy(src, dst, own_sem.at[len(own)]))
        for cp in own:
            cp.start()
        for cp in own:
            cp.wait()

        def p_hop(d):
            lo, hi = around(d)
            v_lo, v_hi = pg.at[lo, core], pg.at[hi, core]
            same(v_lo, p_zsend, p_zrecv.at[0, d - 1], up_z).wait_recv()
            if d < far:
                same(v_lo, p_zsend, p_zrecv.at[0, d], up_z).start()
                same(v_hi, p_zsend, p_zrecv.at[1, d - 1], dn_z).wait_recv()
            if d < far - 1:
                same(v_hi, p_zsend, p_zrecv.at[1, d], dn_z).start()
            same(v_lo, p_dsend, p_drecv, sib).start()
            if d < far:
                same(v_hi, p_dsend, p_drecv, sib).start()

        for t in range(far + 1):
            if t < far:
                p_hop(t + 1)
            for k in range(4):
                slot(t, k)

        p_all = pg.at[:, 1 - core]
        same(p_all, p_dsend, p_drecv, sib).wait_recv()
        low = lax.broadcasted_iota(jnp.int32, (PAR_ROWS, lanes), 1) < head_dim
        for layer in range(n_layers):
            r0 = layer * PAR_ROWS
            for zz in range(n_z):
                tab[layer, :, zz * lanes:(zz + 1) * lanes] = jnp.where(
                    low, pg[zz, 0, r0:r0 + PAR_ROWS, :], pg[zz, 1, r0:r0 + PAR_ROWS, :])
                for cc in range(2):
                    at = (zz * 2 + cc) * down_rows
                    for j in range(down_rows // lanes):
                        r = r0 + 9 + j
                        tab_up[layer, 0:1, at + j * lanes:at + (j + 1) * lanes] = pg[zz, cc, r:r + 1, :]
            for b in range(3 * n_z):
                two = []
                for p in (2 * b, 2 * b + 1):
                    dev, r = p // 3, r0 + 4 + p % 3
                    two.append(pg[dev // 2, dev % 2, r:r + 1, :])
                c0 = (b % n_z) * lanes
                tab[layer, 4 + b // n_z:5 + b // n_z, c0:c0 + lanes] = jnp.where(low[0:1], two[0], two[1])

        def norms(layer, r):
            @pl.loop(0, blk // 64)
            def _(t):
                rows = pl.ds(pl.multiple_of(r * blk + t * 64, 64), 64)
                xf = x_s[rows, :].astype(F32)
                mean = jnp.mean(xf, axis=-1, keepdims=True)
                cen = xf - mean
                var = jnp.mean(cen * cen, axis=-1, keepdims=True)
                nrm = cen * lax.rsqrt(var + LN_EPS)
                a_s[rows, :] = (nrm * tab[layer, 0:1, :] + tab[layer, 1:2, :]).astype(BF)
                m_s[rows, :] = (nrm * tab[layer, 2:3, :] + tab[layer, 3:4, :]).astype(BF)

        def dot(a, b):
            return jnp.dot(a, b, preferred_element_type=F32)

        def rows_of(r):
            return pl.ds(pl.multiple_of(r * blk, blk), blk)

        def w_tile(slot, c0, nc):
            return w_s[slot, :, :, :, c0:c0 + nc].reshape(d_model, nc)

        def qkv_block(layer, j, slot, r):
            rows = rows_of(r)
            for c0 in range(0, d_model, TILE):
                y = dot(a_s[rows, :], w_tile(slot, c0, TILE)) + tab[layer, pl.ds(4 + j, 1), c0:c0 + TILE]
                qkv_s[j, rows, c0:c0 + TILE] = y.astype(BF)

        def attend(n):
            rows = pl.ds(pl.multiple_of(n * seq_len, seq_len), seq_len)
            pos_q = lax.broadcasted_iota(jnp.int32, (seq_len, seq_len), 0)
            pos_k = lax.broadcasted_iota(jnp.int32, (seq_len, seq_len), 1)
            vis = pos_q <= jnp.minimum(pos_k, lens_ref[n] - 1)
            lane = lax.broadcasted_iota(jnp.int32, (seq_len, lanes), 1)
            first = lane < head_dim
            front = lax.rem(lane, 2 * half_rot) < half_rot
            zero = jnp.zeros((seq_len, lanes), BF)

            def rope(u, turn):
                v = pltpu.roll(u, turn, 1) if turn else u
                moved = jnp.where(front, pltpu.roll(u, (turn - half_rot) % lanes, 1), pltpu.roll(u, turn + half_rot, 1))
                return (v.astype(F32) * rope_ref[0] + moved.astype(F32) * rope_ref[1]).astype(BF)

            for p in range(n_heads // 2):
                cs = slice(p * lanes, (p + 1) * lanes)
                trio = []
                for b in range(3 * p, 3 * p + 3):
                    trio.append(qkv_s[b // n_z, rows, (b % n_z) * lanes:(b % n_z + 1) * lanes])
                q_r[:, cs] = rope(jnp.where(first, trio[0], trio[1]), 0)
                k_r[:, cs] = rope(jnp.where(first, trio[2], trio[0]), head_dim)
                v_r[:, cs] = jnp.where(first, trio[1], trio[2])

            for p in range(n_heads // 2):
                cs = slice(p * lanes, (p + 1) * lanes)
                q2, v2 = q_r[:, cs], v_r[:, cs]
                qq = jnp.concatenate([jnp.where(first, q2, zero), jnp.where(first, zero, q2)], axis=0)
                sc = lax.dot_general(k_r[:, cs], qq, (((1,), (1,)), ((), ())), preferred_element_type=F32)
                ctx = []
                for j, vj in enumerate((jnp.where(first, v2, zero), jnp.where(first, zero, v2))):
                    s1 = jnp.where(vis, sc[:, j * seq_len:(j + 1) * seq_len] * (head_dim ** -0.5 * math.log2(math.e)), -1e30)
                    e = jnp.exp2(s1 - jnp.max(s1, axis=0, keepdims=True))
                    pr = (e * (1.0 / jnp.sum(e, axis=0, keepdims=True))).astype(BF)
                    ctx.append(lax.dot_general(pr, vj, (((0,), (0,)), ((), ())), preferred_element_type=F32))
                ctx_s[rows, cs] = (ctx[0] + ctx[1]).astype(BF)

        def out_block(layer, slot, r):
            rows = rows_of(r)
            for c0 in range(0, d_model, TILE):
                cols = slice(c0, c0 + TILE)
                o = dot(ctx_s[rows, :], w_tile(slot, c0, TILE)) + tab[layer, 7:8, cols]
                acc_s[rows, cols] = x_s[rows, cols].astype(F32) + o

        def up_block(layer, j, slot, r):
            rows = rows_of(r)
            for c0 in range(0, d_model, TILE):
                cols = pl.ds(pl.multiple_of(j * d_model + c0, TILE), TILE)
                u = dot(m_s[rows, :], w_tile(slot, c0, TILE)) + tab_up[layer, 0:1, cols]
                act_s[rows, cols] = (u * 0.5 * (1.0 + lax.erf(u * (2.0 ** -0.5)))).astype(BF)

        def down_block(layer, j, slot, r):
            rows = rows_of(r)
            cols = pl.ds(pl.multiple_of(j * d_cols, d_cols), d_cols)
            w = wd_s[slot].reshape(ff, d_cols)
            y = acc_s[rows, cols] + (dot(act_s[rows, :], w) + tab[layer, 8:9, cols])
            x_s[rows, cols] = y.astype(BF)

        def out_copy(j):
            cols = pl.ds(pl.multiple_of(j * d_cols, d_cols), d_cols)
            return pltpu.make_async_copy(x_s.at[:, cols], out_hbm.at[:, cols], out_sem.at[j])

        x_copy.wait()

        @pl.loop(0, n_layers)
        def _(layer):
            s0 = layer * per_layer

            @pl.loop(0, BLOCKS)
            def _(r):
                slots_at(layer, r)

                @pl.when(r == 1)
                def _():
                    fetch(s0, 0)

                norms(layer, r)

            @pl.loop(0, 3)
            def _(j):
                buf = lax.rem(j, 2)

                @pl.loop(0, BLOCKS)
                def _(r):
                    slots_at(layer, BLOCKS * (j + 1) + r)

                    @pl.when(r == 0)
                    def _():
                        loads(s0 + j, buf, False)[0].wait()

                    @pl.when(r == 1)
                    def _():
                        fetch(s0 + j + 1, 1 - buf)

                    qkv_block(layer, j, buf, r)

            @pl.loop(0, docs)
            def _(n):
                slots_at(layer, 4 * BLOCKS + n)

                @pl.when(n == docs - 2)
                def _():
                    fetch(s0 + 4, 0)

                attend(n)

            loads(s0 + 3, 1, False)[0].wait()

            @pl.loop(0, BLOCKS)
            def _(r):
                slots_at(layer, 4 * BLOCKS + docs + r)
                out_block(layer, 1, r)

            @pl.loop(0, n_up)
            def _(j):
                buf = lax.rem(j, 2)

                @pl.loop(0, BLOCKS)
                def _(r):
                    slots_at(layer, (5 + j) * BLOCKS + docs + r)

                    @pl.when(r == 0)
                    def _():
                        loads(s0 + 4 + j, buf, False)[0].wait()

                    @pl.when((r == 1) & (j < n_up - 1))
                    def _():
                        fetch(s0 + 5 + j, 1 - buf)

                    @pl.when((r == 1) & (j == n_up - 1))
                    def _():
                        fetch(s0 + 4 + n_up, 0, True)

                    up_block(layer, j, buf, r)

            @pl.loop(0, n_up)
            def _(j):
                buf = lax.rem(j, 2)

                @pl.loop(0, BLOCKS)
                def _(r):
                    slots_at(layer, (5 + n_up + j) * BLOCKS + docs + r)

                    @pl.when(r == 0)
                    def _():
                        for cp in loads(s0 + 4 + n_up + j, buf, True):
                            cp.wait()

                    @pl.when((r == 1) & (j < n_up - 1))
                    def _():
                        fetch(s0 + 5 + n_up + j, 1 - buf, True)

                    down_block(layer, j, buf, r)

                @pl.when(layer == n_layers - 1)
                def _():
                    out_copy(j).start()

        @pl.loop(0, n_st)
        def _(s):
            sevenths = g.at[s, pl.ds(0, n_z - 1), 0, pl.ds(0, half), :]
            same(sevenths, z_send.at[s], z_recv.at[s, 0, 0], up_z).wait_send()
            same(sevenths, c_send.at[s], z_recv.at[s, 0, 0], up_z).wait_send()
            same(g.at[s, :, 0], d_send.at[s], d_recv.at[s], sib).wait_send()

        seven = pg.at[pl.ds(0, n_z - 1), 0]
        same(seven, p_zsend, p_drecv, up_z).wait_send()
        eight = pg.at[:, 0]
        same(eight, p_dsend, p_drecv, sib).wait_send()
        for j in range(n_up):
            out_copy(j).wait()

    out_shape = (
        jax.ShapeDtypeStruct((tokens, d_model), BF),
        jax.ShapeDtypeStruct((n_st, n_z, 2, rows_w, d_model), BF),
    )
    dma = pltpu.SemaphoreType.DMA
    n_own = n_layers * (4 + n_up + n_up * parts)
    act = pltpu.VMEM((tokens, d_model), BF)
    doc_v = pltpu.VMEM((seq_len, d_model), BF)
    scratch = [
        pltpu.VMEM((n_layers * PAR_ROWS, lanes), F32), act, act, act, doc_v, doc_v, doc_v, pltpu.VMEM((3, tokens, d_model), BF), act, pltpu.VMEM((tokens, ff), BF),
        pltpu.VMEM((tokens, d_model), F32),
        pltpu.VMEM((2, n_z, 2, rows_w, d_model), BF), pltpu.VMEM((2, n_z, 2, down_rows, d_cols), BF),
        pltpu.VMEM((n_layers, rows_w, 3 * d_model), BF), pltpu.VMEM((n_layers, rows_w, d_model), BF),
        pltpu.VMEM((n_layers, rows_w, ff), BF), pltpu.VMEM((n_layers, down_rows, d_model), BF),
        pltpu.VMEM((n_z, 2, n_layers * PAR_ROWS, lanes), F32),
        pltpu.VMEM((n_layers, PAR_ROWS, d_model), F32), pltpu.VMEM((n_layers, 8, ff), F32),
        dma((n_st,)), dma((n_st,)), dma((n_st,)),
        dma((n_st, 2, far)), dma((n_st, 2, far)), dma((n_st, 2, far)), dma((n_st,)),
        dma(()), dma(()), dma((2, far)), dma(()),
        dma(()), dma((4,)), dma((n_own,)), dma((2,)), dma((2, parts)), dma((n_up,)),
    ]
    hbm = pl.BlockSpec(memory_space=pltpu.HBM)
    vmem = pl.BlockSpec(memory_space=pltpu.VMEM)
    smem = pl.BlockSpec(memory_space=pltpu.SMEM)
    return pl.pallas_call(
        kernel,
        name="layers",
        out_shape=out_shape,
        in_specs=[hbm, smem] + [vmem] * 6 + [hbm] * 4,
        out_specs=(hbm, hbm),
        scratch_shapes=scratch,
        compiler_params=pltpu.CompilerParams(collective_id=0, has_side_effects=True, vmem_limit_bytes=67043328),
    )


def solution(mesh):
    row_spec = P(('dp', 'fsdp'), None, None)
    in_specs = (row_spec, P(('dp', 'fsdp')), P(None, None, 'fsdp'), P(None, 'fsdp', None, None), P(None, 'fsdp'), P(None, 'fsdp', None), P(None, 'fsdp'), P(None, 'fsdp', None), P(None, 'fsdp'), P(None, 'fsdp', None), P(None, 'fsdp'))
    n_z = mesh.shape['fsdp'] // 2
    side = math.isqrt(mesh.shape['dp'])

    def local_step(hidden, lens, ln_par, w_qkv, b_qkv, w_out, b_out, w_up, b_up, w_down, b_down):
        docs, seq_len, d_model = hidden.shape
        n_layers, rows, n_heads, triple = w_qkv.shape
        head_dim = triple // 3
        ff = w_up.shape[2]
        wq = w_qkv.reshape(n_layers, rows, n_heads * triple)
        call = make_kernel(n_layers, n_z, side, docs, seq_len, d_model, n_heads, ff)
        out = call(hidden.reshape(docs * seq_len, d_model), lens, ln_par, b_qkv, b_out, b_up, b_down, jnp.asarray(rotary_lanes(seq_len, head_dim)),
                   wq, w_out, w_up, w_down)[0]
        return out.reshape(docs, seq_len, d_model)

    return jax.shard_map(local_step, mesh=mesh, in_specs=in_specs, out_specs=row_spec, check_vma=False)
```
